1024 devices in a mesh: gx: 256 (over y, z, core), gy: 4 (over x).
Axes of the slice: x: 4, y: 4, z: 32, core: 2. Of those that a mesh axis runs over, the one named last changes fastest.
Arguments:
- forcing: float32 [2048, 32, 128], P('gx', 'gy'), may hold values from -12 to 12
- kappa: float32 [256, 4, 16], P('gx', 'gy'), may hold values from 0.25 to 4
- sigma: float32 [256, 4, 16], P('gx', 'gy'), may hold values from 0.5 to 8
Outputs:
- solution: float32 [2048, 32, 128], P('gx', 'gy')
- residual: float32 [2048, 32, 128], P('gx', 'gy')
- rel_residual: float32 [], replicated
The draws below stay inside these ranges and needn't reach their ends.
All inputs are finite; a program needn't handle non-finite values.
Results may differ from the reference program's by a relative error of at most 0.0003.
Values sent between devices are 32-bit elements; how exact they have to be, the bound alone decides.
A program may use at most 64 MiB of HBM per device.

```python
import math
import jax
import jax.numpy as jnp
import numpy as np
from jax import lax

FINE = 8
EZ = 16
NEX = 256
NEY = 4
NODES_X = 2048
NODES_Y = 32
NODES_Z = 128


def draw_forcing(key, part):
    keys = jax.random.split(key, 2)
    shape = (NODES_X, NODES_Y, NODES_Z)
    cells = (NODES_X // FINE, NODES_Y // FINE, NODES_Z // FINE)
    level = 10.0 ** jax.random.uniform(keys[1], cells, jnp.float32)
    level = jnp.repeat(jnp.repeat(jnp.repeat(level, FINE, 0), FINE, 1), FINE, 2)
    across = (jnp.arange(NODES_X, dtype=jnp.float32) / NODES_X)[:, None, None]
    rough = jnp.clip(jax.random.normal(keys[0], shape, jnp.float32), -4.0, 4.0)
    values = 0.1 * rough * level * 3.0 ** across
    return values.astype(jnp.float32)


def steps_of(rng, extent, pieces, least, largest):
    level, own = 1.0, jax.random.fold_in(rng, 6)
    for dim, parts in pieces:
        steps = jnp.exp(jax.random.uniform(jax.random.fold_in(own, dim), (parts,), jnp.float32, least / len(pieces), largest / len(pieces)))
        level = level * jnp.repeat(steps, extent[dim] // parts).reshape([-1 if axis == dim else 1 for axis in range(len(extent))])
    return level


def setup_inputs(seed: int = 0) -> dict:
    key_list = jax.random.split(jax.random.key(seed), 4)
    forcing = draw_forcing(jax.random.fold_in(key_list[3], 71), 0)
    kappa = jnp.clip(jnp.exp(math.log(4.0) - 2.7725887 * jax.random.uniform(key_list[1], (NEX, NEY, EZ), jnp.float32) ** steps_of(key_list[1], (NEX, NEY, EZ), ((0, 256), (1, 4)), -0.2, 0.2)), 0.25, 4.0)
    sigma = jnp.clip(jnp.exp(math.log(8.0) - 2.7725887 * jax.random.uniform(key_list[2], (NEX, NEY, EZ), jnp.float32) ** steps_of(key_list[2], (NEX, NEY, EZ), ((0, 256), (1, 4)), -0.2, 0.2)), 0.5, 8.0)
    return dict(forcing=forcing, kappa=kappa, sigma=sigma)


def legendre_table(points, order):
    columns = [points * 0.0 + 1.0, points]
    for degree in range(2, order + 1):
        columns.append(((2 * degree - 1) * points * columns[-1] - (degree - 1) * columns[-2]) / degree)
    return np.stack(columns, axis=1)

def lobatto(count):
    order = count - 1
    points = np.cos(np.pi * np.arange(count) / order)
    for sweep in range(60):
        table = legendre_table(points, order)
        points = points - (points * table[:, order] - table[:, order - 1]) / (count * table[:, order])
    table = legendre_table(points, order)
    weights = 2.0 / (order * count * table[:, order] ** 2)
    values = table[:, order]
    points, weights, values = (points[::-1], weights[::-1], values[::-1])
    spread = points[:, None] - points[None, :] + np.eye(count)
    deriv = values[:, None] / values[None, :] / spread * (1.0 - np.eye(count))
    corner = order * (order + 1) / 4.0
    ends = np.array([-corner] + [0.0] * (count - 2) + [corner])
    return (points, weights, deriv + np.eye(count) * ends[None, :])

def lagrange(fine_points, coarse_points):
    columns = []
    for column in range(len(coarse_points)):
        value = fine_points * 0.0 + 1.0
        for other in range(len(coarse_points)):
            if other != column:
                value = value * (fine_points - coarse_points[other]) / (coarse_points[column] - coarse_points[other])
        columns.append(value)
    return np.stack(columns, axis=1)

def edge_factor(count, blocks):
    index = jnp.arange(count)
    single = jnp.where((index == 0) | (index == count - 1), 0.5, 1.0).astype(jnp.float32)
    return jnp.tile(single, blocks)

def multiplicity(count, blocks):
    first = edge_factor(count, blocks[0])
    second = edge_factor(count, blocks[1])
    third = edge_factor(count, blocks[2])
    return first[:, None, None] * second[None, :, None] * third[None, None, :]

def element_apply(field, kappa, sigma, deriv, weights):
    count = deriv.shape[0]
    ex, ey, ez = kappa.shape
    high = lax.Precision.HIGHEST
    block = field.reshape(ex, count, ey, count, ez, count)
    mass = (weights[:, None, None] * weights[None, :, None] * weights[None, None, :])[None, :, None, :, None, :]
    first = jnp.einsum('ai,eifjgk->eafjgk', deriv, block, precision=high)
    total = jnp.einsum('ai,eafjgk->eifjgk', deriv, first * mass, precision=high)
    second = jnp.einsum('aj,eifjgk->eifagk', deriv, block, precision=high)
    total = total + jnp.einsum('aj,eifagk->eifjgk', deriv, second * mass, precision=high)
    third = jnp.einsum('ak,eifjgk->eifjga', deriv, block, precision=high)
    total = total + jnp.einsum('ak,eifjga->eifjgk', deriv, third * mass, precision=high)
    coeff = kappa[:, None, :, None, :, None]
    shift = sigma[:, None, :, None, :, None]
    return (coeff * total + shift * mass * block).reshape(field.shape)

def element_diagonal(kappa, sigma, deriv, weights):
    count = deriv.shape[0]
    ex, ey, ez = kappa.shape
    stiff = lax.optimization_barrier(jnp.sum(deriv * deriv * weights[:, None], axis=0))
    term = stiff[:, None, None] * weights[None, :, None] * weights[None, None, :]
    term = term + weights[:, None, None] * stiff[None, :, None] * weights[None, None, :]
    term = term + weights[:, None, None] * weights[None, :, None] * stiff[None, None, :]
    mass = weights[:, None, None] * weights[None, :, None] * weights[None, None, :]
    coeff = kappa[:, None, :, None, :, None]
    shift = sigma[:, None, :, None, :, None]
    full = coeff * term[None, :, None, :, None, :] + shift * mass[None, :, None, :, None, :]
    return full.reshape(ex * count, ey * count, ez * count)

def fold_axis(field, dim, count):
    size = field.shape[dim]
    position = jnp.arange(size) % count
    shape = [1, 1, 1]
    shape[dim] = size
    first = (position == 0).reshape(shape)
    last = (position == count - 1).reshape(shape)
    before = jnp.roll(field, 1, dim)
    after = jnp.roll(field, -1, dim)
    return field + jnp.where(first, before, 0.0) + jnp.where(last, after, 0.0)

def assemble(field, count):
    return fold_axis(fold_axis(fold_axis(field, 0, count), 1, count), 2, count)

def restrict(field, interp, blocks, fine_count, coarse_count):
    high = lax.Precision.HIGHEST
    block = field.reshape(blocks[0], fine_count, blocks[1], fine_count, blocks[2], fine_count)
    one = jnp.einsum('ia,eifjgk->eafjgk', interp, block, precision=high)
    two = jnp.einsum('jb,eafjgk->eafbgk', interp, one, precision=high)
    three = jnp.einsum('kc,eafbgk->eafbgc', interp, two, precision=high)
    return three.reshape(blocks[0] * coarse_count, blocks[1] * coarse_count, blocks[2] * coarse_count)

def prolong(field, interp, blocks, fine_count, coarse_count):
    high = lax.Precision.HIGHEST
    block = field.reshape(blocks[0], coarse_count, blocks[1], coarse_count, blocks[2], coarse_count)
    one = jnp.einsum('ia,eafbgc->eifbgc', interp, block, precision=high)
    two = jnp.einsum('jb,eifbgc->eifjgc', interp, one, precision=high)
    three = jnp.einsum('kc,eifjgc->eifjgk', interp, two, precision=high)
    return three.reshape(blocks[0] * fine_count, blocks[1] * fine_count, blocks[2] * fine_count)

def reference(forcing, kappa, sigma):
    blocks = kappa.shape
    counts = [8, 4, 2]
    tables = [lobatto(count) for count in counts]
    derivs = [jnp.asarray(table[2], jnp.float32) for table in tables]
    weights = [jnp.asarray(table[1], jnp.float32) for table in tables]
    interps = [jnp.asarray(lagrange(tables[level][0], tables[level + 1][0]), jnp.float32) for level in range(2)]
    mults = [multiplicity(count, blocks) for count in counts]
    diags = [assemble(element_diagonal(kappa, sigma, derivs[level], weights[level]), counts[level]) for level in range(3)]
    center = 1.65
    half = 1.35
    ratio = center / half

    def operate(field, level):
        return assemble(element_apply(field, kappa, sigma, derivs[level], weights[level]), counts[level])

    def smooth(resid, level, steps, keep_last):
        rho = 1.0 / ratio
        direction = resid / (center * diags[level])
        iterate = direction
        for step in range(steps):
            if step > 0:
                rho_next = 1.0 / (2.0 * ratio - rho)
                direction = rho_next * rho * direction + 2.0 * rho_next / half * resid / diags[level]
                iterate = iterate + direction
                rho = rho_next
            if step < steps - 1 or keep_last:
                resid = resid - operate(direction, level)
        return (iterate, resid)

    def vcycle(resid, level):
        if level == 2:
            iterate, unused = smooth(resid, level, 2, False)
            return iterate
        iterate, resid = smooth(resid, level, 2, True)
        coarse = assemble(restrict(mults[level] * resid, interps[level], blocks, counts[level], counts[level + 1]), counts[level + 1])
        correction = prolong(vcycle(coarse, level + 1), interps[level], blocks, counts[level], counts[level + 1])
        iterate = iterate + correction
        resid = resid - operate(correction, level)
        return iterate + resid / (center * diags[level])
    load = assemble(forcing, 8)
    first = vcycle(load, 0)
    image_first = operate(first, 0)
    second = vcycle(load - image_first, 0)
    combined = first + second
    image = operate(combined, 0)
    weight = mults[0]
    coef = jnp.sum(weight * load * image) / jnp.sum(weight * image * image)
    solution = coef * combined
    residual = load - coef * image
    rel_residual = jnp.sqrt(jnp.sum(weight * residual * residual) / jnp.sum(weight * load * load))
    return (solution, residual, rel_residual)
```

```python
import jax
import jax.numpy as jnp
import numpy as np
from jax import lax
from jax.experimental import pallas as pl
from jax.experimental.pallas import tpu as pltpu
from jax.sharding import PartitionSpec as P


def legendre_table(points, order):
    columns = [points * 0.0 + 1.0, points]
    for degree in range(2, order + 1):
        columns.append(((2 * degree - 1) * points * columns[-1] - (degree - 1) * columns[-2]) / degree)
    return np.stack(columns, axis=1)

def lobatto(count):
    order = count - 1
    points = np.cos(np.pi * np.arange(count) / order)
    for sweep in range(60):
        table = legendre_table(points, order)
        points = points - (points * table[:, order] - table[:, order - 1]) / (count * table[:, order])
    table = legendre_table(points, order)
    weights = 2.0 / (order * count * table[:, order] ** 2)
    values = table[:, order]
    points, weights, values = (points[::-1], weights[::-1], values[::-1])
    spread = points[:, None] - points[None, :] + np.eye(count)
    deriv = values[:, None] / values[None, :] / spread * (1.0 - np.eye(count))
    corner = order * (order + 1) / 4.0
    ends = np.array([-corner] + [0.0] * (count - 2) + [corner])
    return (points, weights, deriv + np.eye(count) * ends[None, :])

def lagrange(fine_points, coarse_points):
    columns = []
    for column in range(len(coarse_points)):
        value = fine_points * 0.0 + 1.0
        for other in range(len(coarse_points)):
            if other != column:
                value = value * (fine_points - coarse_points[other]) / (coarse_points[column] - coarse_points[other])
        columns.append(value)
    return np.stack(columns, axis=1)

X8, w8, D8 = lobatto(8); X4, w4, D4 = lobatto(4); X2, w2, D2 = lobatto(2)
J1 = lagrange(X8, X4)
J2 = lagrange(X4, X2)
K8, K4, K2 = (D.T @ (w[:, None] * D) for D, w in ((D8, w8), (D4, w4), (D2, w2)))
Kd8, Kd4, Kd2 = (np.diag(K) for K in (K8, K4, K2))
f8 = np.array([.5] + [1.]*6 + [.5]); f4 = np.array([.5, 1, 1, .5])
lane = np.arange(128)[None, :]; sub = np.arange(8)[:, None]
ones = np.ones((8, 128))
T = {}
def put(name, a): T[name] = np.ascontiguousarray(np.broadcast_to(a, (8, 128)).astype(np.float32))
kz = lane % 8
K8s = K8 / w8[:, None]
for d in range(1, 8):
    put(f"cy{d}", K8s[sub, (sub - d) % 8] * ones)
for d in range(-7, 8):
    if d == 0: continue
    src = kz - d; ok = (src >= 0) & (src < 8)
    put(f"cz{d}", np.where(ok, K8s[kz, np.clip(src, 0, 7)], 0.0))
put("cyz0", K8s[sub, sub] + K8s[kz, kz])
put("wyz", w8[sub] * w8[kz])
put("mz0", (kz == 0) * 1.0); put("mz7", (kz == 7) * 1.0)
put("jm0", (sub == 0) * 1.0); put("jm7", (sub == 7) * 1.0)
for i in range(4):
    put(f"gk{i}", (Kd8[i] * w8[sub] + w8[i] * Kd8[sub]) * w8[kz] + w8[i] * w8[sub] * Kd8[kz])
    put(f"gw{i}", w8[i] * w8[sub] * w8[kz])
put("m8", f8[sub] * f8[kz])
i4 = sub // 2; jp = sub % 2; h = lane % 2; k4 = (lane % 8) // 2; j4 = 2 * jp + h
for j in range(8):
    for hh in range(2):
        put(f"ry{j}_{hh}", J1[j, 2 * jp + hh] * ones)
RZ = []
for hh in range(2):
    for d in range(-7, 8):
        src = (lane % 8) - d; ok = (src >= 0) & (src < 8) & (h == hh)
        c = np.where(ok, J1[np.clip(src, 0, 7), k4], 0.0)
        if np.any(c != 0): put(f"rz{hh}_{d}", c); RZ.append((hh, d))
PZ = {}
for d in range(-7, 8):
    for hh in range(2):
        src = kz - d; ok = (src >= 0) & (src < 8) & (src % 2 == hh)
        c = np.where(ok, J1[kz, np.clip(src // 2, 0, 3)], 0.0)
        if np.any(c != 0): put(f"pz{hh}_{d}", c); PZ.setdefault(d, []).append(hh)
for b in range(4): put(f"py{b}", J1[sub, b] * ones)
def ops4(tag, M, dirs):
    M = np.asarray(M)
    if "x" in dirs:
        for d in range(4): put(f"{tag}x{d}", M[i4, (i4 - d) % 4] * ones)
    if "y" in dirs:
        put(f"{tag}ya", M[j4, j4]); put(f"{tag}yb", M[j4, 2 * (1 - jp) + h])
        put(f"{tag}yc", M[2 * jp + 1 - h, j4]); put(f"{tag}yd", M[2 * jp + 1 - h, 2 * (1 - jp) + h])
    if "z" in dirs:
        for d in range(-3, 4):
            src = k4 - d; ok = (src >= 0) & (src < 4)
            put(f"{tag}z{d}", np.where(ok, M[k4, np.clip(src, 0, 3)], 0.0))
K4s = K4 / w4[:, None]
for t in ("x", "y", "z"): ops4("a", K4s, t)
put("a0", K4s[i4, i4] + K4s[j4, j4] + K4s[k4, k4])
put("W1", w4[i4] * w4[j4] * w4[k4])
put("G1", Kd4[i4] * w4[j4] * w4[k4] + w4[i4] * Kd4[j4] * w4[k4] + w4[i4] * w4[j4] * Kd4[k4])
put("m1", f4[i4] * f4[j4] * f4[k4])
put("z0", (k4 == 0) * 1.0); put("z3", (k4 == 3) * 1.0)
put("x0", (i4 == 0) * 1.0); put("x3", (i4 == 3) * 1.0)
put("y0", (j4 == 0) * 1.0); put("y3", (j4 == 3) * 1.0)
cor = lambda a: (a == 0) | (a == 3)
cmask = (cor(i4) & cor(j4) & cor(k4)) * 1.0
R2 = np.zeros((4, 4)); R2[0] = J2[:, 0]; R2[3] = J2[:, 1]
P2 = np.zeros((4, 4)); P2[:, 0] = J2[:, 0]; P2[:, 3] = J2[:, 1]
K2s = K2 / w2[:, None]
B2 = np.zeros((4, 4)); B2[np.ix_([0, 3], [0, 3])] = K2s
for t in ("x", "y", "z"):
    ops4("r", R2, t); ops4("p", P2, t); ops4("b", B2, t)
w2e = np.array([w2[0], 0, 0, w2[1]]); Kd2e = np.array([Kd2[0], 0, 0, Kd2[1]])
put("W2", w2e[i4] * w2e[j4] * w2e[k4])
put("G2", Kd2e[i4] * w2e[j4] * w2e[k4] + w2e[i4] * Kd2e[j4] * w2e[k4] + w2e[i4] * w2e[j4] * Kd2e[k4])
put("off2", 1.0 - cmask)
NZ_ = lambda n: np.any(T[n] != 0)
THETA, DELTA = 1.65, 1.35
S_ = THETA / DELTA; rho0 = 1 / S_; rho1 = 1 / (2 * S_ - rho0)
ALPHA = rho1 * rho0; BETA = 2 * rho1 / DELTA

NAMES = [n for n in T if np.any(T[n])]
INDEX = {n: k for k, n in enumerate(NAMES)}
TABLE = np.stack([T[n] for n in NAMES])
K8 = [[float(np.float32(x)) for x in r] for r in K8]
w8 = [float(np.float32(x)) for x in w8]


def live(name):
    return name in INDEX


def lr(v, s):
    return pltpu.roll(v, s % 128, 1)


def sr(v, s):
    return pltpu.roll(v, s % 8, 0)


def halves():
    s = lax.broadcasted_iota(jnp.int32, (8, 128), 0)
    l = lax.broadcasted_iota(jnp.int32, (8, 128), 1)
    return s % 2 == 1, l % 2 == 1

def zops(C, tag, v, skip0=False):
    out = None
    for d in range(-3, 4):
        if (d == 0 and skip0) or not live(f"{tag}z{d}"): continue
        t = C(f"{tag}z{d}") * (lr(v, 2 * d) if d else v)
        out = t if out is None else out + t
    return out

def xops(C, tag, v, skip0=False):
    out = None
    for d in range(4):
        if (d == 0 and skip0) or not live(f"{tag}x{d}"): continue
        t = C(f"{tag}x{d}") * (sr(v, 2 * d) if d else v)
        out = t if out is None else out + t
    return out

def yops(C, tag, v, skip0=False):
    jp1, h1 = halves()
    sw = jnp.where(jp1, sr(v, 1), sr(v, -1)) if live(f"{tag}yb") or live(f"{tag}yd") else None
    def pair(a, b):
        t = None
        if live(a): t = C(a) * v
        if live(b): t = C(b) * sw if t is None else t + C(b) * sw
        return t
    other = pair(f"{tag}yc", f"{tag}yd")
    out = None if other is None else jnp.where(h1, lr(other, 1), lr(other, -1))
    if skip0:
        if live(f"{tag}yb"): out = out + C(f"{tag}yb") * sw
        return out
    same = pair(f"{tag}ya", f"{tag}yb")
    return same if out is None else (out if same is None else out + same)

def a1(C, v, kap, sig):
    k = C("a0") * v + xops(C, "a", v, True) + yops(C, "a", v, True) + zops(C, "a", v, True)
    return C("W1") * (kap * k + sig * v)

def a2(C, v, kap, sig):
    k = xops(C, "b", v) + yops(C, "b", v) + zops(C, "b", v)
    return C("W2") * (kap * k + sig * v)

def restrict2(C, v): return zops(C, "r", yops(C, "r", xops(C, "r", v)))
def prolong2(C, v): return xops(C, "p", yops(C, "p", zops(C, "p", v)))
def sz1(C, v): return v + C("z0") * lr(v, 2) + C("z3") * lr(v, -2)
def xfrom_l(C, v): return C("x0") * sr(v, 2)
def xfrom_r(C, v): return C("x3") * sr(v, -2)
def yfrom_l(C, v): return C("y0") * lr(sr(v, -1), -1)
def yfrom_r(C, v): return C("y3") * lr(sr(v, 1), 1)

def a_fine(C, v, c1, rho):
    e = C("cyz0") + rho
    out = []
    for i in range(8):
        t = e * v[i]
        for d in range(1, 8): t = t + C(f"cy{d}") * sr(v[i], d)
        for d in range(-7, 8):
            if d: t = t + C(f"cz{d}") * lr(v[i], d)
        x = K8[i][0] * v[0]
        for a in range(1, 8): x = x + K8[i][a] * v[a]
        out.append(c1 * (x + w8[i] * t))
    return out

def sz8(C, v): return v + C("mz0") * lr(v, 1) + C("mz7") * lr(v, -1)

MESH = pl.DeviceIdType.MESH
NY = 4
ZR = 32
YR = 4
GX = ZR * YR * 2
R = 5
NC = (2 * R + 1) * NY
OWN = R * NY
PARTNERS = [(dx, dy) for dx in range(-R, R + 1) for dy in range(NY) if (dx, dy) != (0, 0)]
ROUNDS = 7
TI = 1.0 / THETA


def slot(dx, dy):
    return (dx + R) * NY + dy % NY


def kernel(tab_hbm, forc, kap_in, sig_in, one_hot, sol, res, rel,
           tab, V, ks_s, KS, SX, SY, SC, RX, RY, RC, ID0, B, D0, R1, Q, XS,
           us, U, ID1, ID2, C1B, D0B, VA, R1B, D1B, VB, C2B, G0B, QB, VC, X1,
           ap, AZ, pp, AP,
           tab_sem, ks_send, ks_recv, f_send, f_recv, u_send, u_recv,
           z_send, z_recv, p_send, p_recv, chain):
    gx = lax.axis_index("gx")
    gy = lax.axis_index("gy")
    core = lax.rem(gx, 2)
    zc = lax.rem(gx // 2, ZR)
    yc = gx // (2 * ZR)

    def at(dx, dy):
        return (lax.rem(gx + dx + GX, GX), lax.rem(gy + dy + NY, NY))

    def zring(k):
        return (yc * (2 * ZR) + 2 * lax.rem(zc + k + ZR, ZR) + core, gy)

    def plane(dy, dc, dx):
        return (lax.rem(yc + dy, YR) * (2 * ZR) + 2 * zc + lax.rem(core + dc, 2), lax.rem(gy + dx, NY))

    def C(name):
        return tab[INDEX[name]]

    tab_copy = pltpu.make_async_copy(tab_hbm, tab, tab_sem)
    tab_copy.start()

    barrier = pltpu.get_barrier_semaphore()
    greet = [at(dx, dy) for dx, dy in PARTNERS]
    greet += [zring(k) for k in (-3, -2, -1, 1, 2, 3)] + [plane(k, 0, 0) for k in (1, 2, 3)]
    for d in greet:
        pl.semaphore_signal(barrier, inc=1, device_id=d, device_id_type=MESH)

    hot = one_hot[...]
    def lanes(ref):
        return jnp.dot(jnp.broadcast_to(ref[...], (8, 16)), hot, precision=lax.Precision.HIGHEST, preferred_element_type=jnp.float32)
    kap = lanes(kap_in)
    sig = lanes(sig_in)
    ks_s[0:1] = kap[0:1]
    ks_s[1:2] = sig[0:1]
    KS[OWN, 0:1] = kap[0:1]
    KS[OWN, 1:2] = sig[0:1]
    tab_copy.wait()

    def put_faces(rnd):
        SX[rnd, 0] = V[0:8]
        SX[rnd, 1] = V[56:64]
        SY[rnd, 0] = V[pl.ds(0, 8, stride=8)]
        SY[rnd, 1] = V[pl.ds(7, 8, stride=8)]
        for k, row in enumerate((0, 7, 56, 63)):
            SC[rnd, k] = V[row:row + 1]

    def face_copies(rnd):
        out = []
        for s in range(2):
            step = 2 * s - 1
            out.append((SX.at[rnd, s], RX.at[rnd, 1 - s], at(step, 0)))
        for s in range(2):
            step = 2 * s - 1
            out.append((SY.at[rnd, s], RY.at[rnd, 1 - s], at(0, step)))
        for k in range(4):
            out.append((SC.at[rnd, k], RC.at[rnd, 3 - k], at(2 * (k // 2) - 1, 2 * (k % 2) - 1)))
        return [pltpu.make_async_remote_copy(src_ref=a, dst_ref=b, send_sem=f_send.at[rnd, n], recv_sem=f_recv.at[rnd, RSEM[n]],
                                             device_id=d, device_id_type=MESH) for n, (a, b, d) in enumerate(out)]

    def face_start(rnd, tiles):
        for i in range(8):
            V[8 * i:8 * i + 8] = tiles[i]
        put_faces(rnd)
        for c in face_copies(rnd):
            c.start()

    def face_wait(rnd):
        for n in range(8):
            pltpu.make_async_remote_copy(src_ref=(RX.at[rnd, n] if n < 2 else RY.at[rnd, n - 2] if n < 4 else RC.at[rnd, n - 4]),
                                         dst_ref=(RX.at[rnd, n] if n < 2 else RY.at[rnd, n - 2] if n < 4 else RC.at[rnd, n - 4]),
                                         send_sem=f_send.at[rnd, n], recv_sem=f_recv.at[rnd, n], device_id=at(1, 0), device_id_type=MESH).wait_recv()
        V[0:8] = V[0:8] + RX[rnd, 0]
        V[56:64] = V[56:64] + RX[rnd, 1]
        V[pl.ds(0, 8, stride=8)] = V[pl.ds(0, 8, stride=8)] + RY[rnd, 0]
        V[pl.ds(7, 8, stride=8)] = V[pl.ds(7, 8, stride=8)] + RY[rnd, 1]
        for k, row in enumerate((0, 7, 56, 63)):
            V[row:row + 1] = V[row:row + 1] + RC[rnd, k]
        return [V[8 * i:8 * i + 8] for i in range(8)]

    pl.semaphore_wait(barrier, len(greet))

    face_start(0, [sz8(C, forc[i]) for i in range(8)])
    def ks_copy(dx, dy):
        return pltpu.make_async_remote_copy(src_ref=ks_s, dst_ref=KS.at[slot(-dx, -dy)], send_sem=ks_send, recv_sem=ks_recv,
                                            device_id=at(dx, dy), device_id_type=MESH)
    for dx, dy in PARTNERS:
        ks_copy(dx, dy).start()
    for k in (-3, 3):
        pl.semaphore_signal(chain.at[0], inc=1, device_id=zring(k), device_id_type=MESH)
    for k in (1, 2, 3):
        pl.semaphore_signal(chain.at[3], inc=1, device_id=plane(k, 0, 0), device_id_type=MESH)

    def all_but_one(buf, send, recv):
        return pltpu.make_async_remote_copy(src_ref=buf.at[pl.ds(0, NC - 1)], dst_ref=buf.at[pl.ds(0, NC - 1)], send_sem=send, recv_sem=recv,
                                            device_id=at(1, 0), device_id_type=MESH)

    b = face_wait(0)
    for i in range(8):
        B[i] = b[i]
        R1[i] = b[i]
        XS[i] = jnp.zeros((8, 128), jnp.float32)
    all_but_one(KS, ks_send, ks_recv).wait_recv()

    def row(dx, dy, which):
        return KS[slot(dx, dy), which:which + 1]
    prof = [[], []]
    for dx in (-1, 0, 1):
        for which in range(2):
            prof[which].append(row(dx, 0, which) + C("jm0") * row(dx, -1, which) + C("jm7") * row(dx, 1, which))
    for i in range(8):
        kk, ss = prof[0][1], prof[1][1]
        if i == 0:
            kk, ss = kk + prof[0][0], ss + prof[1][0]
        if i == 7:
            kk, ss = kk + prof[0][2], ss + prof[1][2]
        ii = min(i, 7 - i)
        ID0[i] = 1.0 / sz8(C, kk * C(f"gk{ii}") + ss * C(f"gw{ii}"))

    def kap_of(dx, dy):
        return KS[(dx + R) * NY + dy, 0:1]

    def sig_of(dx, dy):
        return KS[(dx + R) * NY + dy, 1:2]

    def assembled(buf, dx):
        base = (dx + R) * NY
        u = [buf[base + dy] + xfrom_l(C, buf[base - NY + dy]) + xfrom_r(C, buf[base + NY + dy]) for dy in range(NY)]
        up = [yfrom_l(C, u[dy]) for dy in range(NY)]
        dn = [yfrom_r(C, u[dy]) for dy in range(NY)]
        return [u[dy] + up[(dy - 1) % NY] + dn[(dy + 1) % NY] for dy in range(NY)]

    def over(radius, body):
        def go(n, carry):
            body(n - radius)
            return carry
        lax.fori_loop(0, 2 * radius + 1, go, 0)

    def g_one(dx):
        for dy in range(NY):
            c = (dx + R) * NY + dy
            VA[c] = sz1(C, kap_of(dx, dy) * C("G1") + sig_of(dx, dy) * C("W1"))
            VB[c] = sz1(C, kap_of(dx, dy) * C("G2") + sig_of(dx, dy) * C("W2"))
    over(R, g_one)
    def g_two(dx):
        s1, s2 = assembled(VA, dx), assembled(VB, dx)
        for dy in range(NY):
            c = (dx + R) * NY + dy
            ID1[c] = 1.0 / s1[dy]
            ID2[c] = 1.0 / (s2[dy] + C("off2"))
    over(R - 1, g_two)

    pl.semaphore_wait(chain.at[0], 2)
    for k in (-6, 6):
        pl.semaphore_signal(chain.at[1], inc=1, device_id=zring(k), device_id_type=MESH)

    c1 = kap * C("wyz")
    rho = sig / kap

    def tiles(ref):
        return [ref[i] for i in range(8)]

    def u_copy(cyc, dx, dy):
        return pltpu.make_async_remote_copy(src_ref=us.at[cyc], dst_ref=U.at[cyc, slot(-dx, -dy)], send_sem=u_send.at[cyc], recv_sem=u_recv.at[cyc],
                                            device_id=at(dx, dy), device_id_type=MESH)

    def coarse(cyc):
        Uc = U.at[cyc]
        def first(dx):
            s = assembled(Uc, dx)
            for dy in range(NY):
                c = (dx + R) * NY + dy
                d0 = TI * s[dy] * ID1[c]
                C1B[c] = s[dy]
                D0B[c] = d0
                VA[c] = sz1(C, a1(C, d0, kap_of(dx, dy), sig_of(dx, dy)))
        over(R - 1, first)
        def second(dx):
            s = assembled(VA, dx)
            for dy in range(NY):
                c = (dx + R) * NY + dy
                r1 = C1B[c] - s[dy]
                d1 = ALPHA * D0B[c] + BETA * r1 * ID1[c]
                t = C("m1") * r1 - a1(C, d1, kap_of(dx, dy), sig_of(dx, dy))
                R1B[c] = r1
                D1B[c] = d1
                VB[c] = sz1(C, restrict2(C, t))
        over(R - 2, second)
        def third(dx):
            s = assembled(VB, dx)
            for dy in range(NY):
                c = (dx + R) * NY + dy
                g0 = TI * s[dy] * ID2[c]
                C2B[c] = s[dy]
                G0B[c] = g0
                VA[c] = sz1(C, a2(C, g0, kap_of(dx, dy), sig_of(dx, dy)))
        over(R - 3, third)
        def fourth(dx):
            s = assembled(VA, dx)
            for dy in range(NY):
                c = (dx + R) * NY + dy
                x2 = (1.0 + ALPHA) * G0B[c] + BETA * (C2B[c] - s[dy]) * ID2[c]
                q = D1B[c] + prolong2(C, x2)
                QB[c] = q
                VC[c] = sz1(C, a1(C, q, kap_of(dx, dy), sig_of(dx, dy)))
        over(R - 4, fourth)
        s = assembled(VC, 0)
        for dy in range(1):
            c = OWN + dy
            X1[dy] = D0B[c] + QB[c] + TI * (R1B[c] - s[dy]) * ID1[c]

    def restrict1(t):
        xs = [sum(float(J1[i, a]) * t[i] for i in range(8)) for a in range(4)]
        for s in range(8):
            V[8 * s:8 * s + 8] = xs[s // 2]
        out = None
        for hh in range(2):
            y = None
            for j in range(8):
                if live(f"ry{j}_{hh}"):
                    p = C(f"ry{j}_{hh}") * V[pl.ds(j, 8, stride=8)]
                    y = p if y is None else y + p
            for h2, d in RZ:
                if h2 == hh:
                    p = C(f"rz{hh}_{d}") * (lr(y, d) if d else y)
                    out = p if out is None else out + p
        return out

    def prolong1(e):
        z = [None, None]
        for d in PZ:
            r = lr(e, d) if d else e
            for hh in PZ[d]:
                p = C(f"pz{hh}_{d}") * r
                z[hh] = p if z[hh] is None else z[hh] + p
        V[0:8] = z[0]
        V[8:16] = z[1]
        ex = []
        for a in range(4):
            ex.append(sum(C(f"py{bb}") * V[pl.ds((bb % 2) * 8 + 2 * a + bb // 2, 8, stride=0)] for bb in range(4)))
        return [sum(float(J1[i, a]) * ex[a] for a in range(4)) for i in range(8)]

    def apply(rnd, v):
        face_start(rnd, [sz8(C, t) for t in a_fine(C, v, c1, rho)])
        return face_wait(rnd)

    def cycle(cyc, carry):
        rnd = 1 + 3 * cyc
        r = tiles(R1)
        d0 = [TI * r[i] * ID0[i] for i in range(8)]
        for i in range(8):
            D0[i] = d0[i]
        s = apply(rnd, d0)
        d1, t = [], []
        for i in range(8):
            r1 = R1[i] - s[i]
            R1[i] = r1
            d1.append(ALPHA * D0[i] + BETA * r1 * ID0[i])
            Q[i] = d1[i]
        w = a_fine(C, d1, c1, rho)
        t = [float(f8[i]) * C("m8") * R1[i] - w[i] for i in range(8)]
        u = sz1(C, restrict1(t))
        us[cyc] = u
        U[cyc, OWN] = u
        for dx, dy in PARTNERS:
            u_copy(cyc, dx, dy).start()
        @pl.when(cyc == 0)
        def _():
            pl.semaphore_wait(chain.at[1], 2)
            for k in (-10, 10):
                pl.semaphore_signal(chain.at[2], inc=1, device_id=zring(k), device_id_type=MESH)
        all_but_one(U.at[cyc], u_send.at[cyc], u_recv.at[cyc]).wait_recv()
        coarse(cyc)
        e = prolong1(X1[0])
        q = [Q[i] + e[i] for i in range(8)]
        for i in range(8):
            Q[i] = q[i]
        s = apply(rnd + 1, q)
        dl = []
        for i in range(8):
            r3 = R1[i] - s[i]
            R1[i] = r3
            x = TI * r3 * ID0[i]
            dl.append(x)
            XS[i] = XS[i] + (D0[i] + Q[i] + x)
        s = apply(rnd + 2, dl)
        for i in range(8):
            R1[i] = R1[i] - s[i]
        return carry

    lax.fori_loop(0, 2, cycle, 0)

    def dot(p, q):
        t = sum(float(f8[i]) * C("m8") * p[i] * q[i] for i in range(8))
        return jnp.sum(jnp.sum(t, axis=1, keepdims=True), axis=0, keepdims=True)
    ln = lax.broadcasted_iota(jnp.int32, (1, 128), 1)
    mine = jnp.where(ln == 0, dot(B, B), jnp.where(ln == 1, dot(B, R1), dot(R1, R1)))
    ap[...] = mine
    AZ[zc] = mine
    pl.semaphore_wait(chain.at[2], 2)
    pl.semaphore_wait(chain.at[3], 3)
    def z_copy(k):
        return pltpu.make_async_remote_copy(src_ref=ap, dst_ref=AZ.at[zc], send_sem=z_send, recv_sem=z_recv, device_id=zring(k), device_id_type=MESH)
    for k in range(1, ZR // 2):
        z_copy(k).start()
        z_copy(-k).start()
    z_copy(ZR // 2).start()
    def most(buf, send, recv):
        return pltpu.make_async_remote_copy(src_ref=buf.at[pl.ds(0, 31)], dst_ref=buf.at[pl.ds(0, 31)], send_sem=send, recv_sem=recv,
                                            device_id=at(1, 0), device_id_type=MESH)
    most(AZ, z_send, z_recv).wait_recv()
    part = AZ[0]
    for k in range(1, ZR):
        part = part + AZ[k]
    pp[...] = part
    pi = yc * 8 + gy * 2 + core
    AP[pi] = part
    others = [(a, c, x) for a in range(YR) for c in range(2) for x in range(NY) if (a, c, x) != (0, 0, 0)]
    def p_copy(o):
        return pltpu.make_async_remote_copy(src_ref=pp, dst_ref=AP.at[pi], send_sem=p_send, recv_sem=p_recv, device_id=plane(*o), device_id_type=MESH)
    for o in others:
        p_copy(o).start()
    most(AP, p_send, p_recv).wait_recv()
    tot = AP[0]
    for k in range(1, 32):
        tot = tot + AP[k]
    bb, br, rr = tot[0:1, 0:1], tot[0:1, 1:2], tot[0:1, 2:3]
    ww = bb - 2.0 * br + rr
    coef = (bb - br) / ww
    for i in range(8):
        sol[i] = coef * XS[i]
        res[i] = B[i] - coef * (B[i] - R1[i])
    rel[...] = jnp.broadcast_to(jnp.sqrt((bb * rr - br * br) / (ww * bb)), (1, 128))

    most(AP, p_send, p_recv).wait_send()
    most(AZ, z_send, z_recv).wait_send()
    all_but_one(KS, ks_send, ks_recv).wait_send()
    for cyc in range(2):
        all_but_one(U.at[cyc], u_send.at[cyc], u_recv.at[cyc]).wait_send()
    for rnd in range(ROUNDS):
        for c in face_copies(rnd):
            c.wait_send()


RSEM = [1, 0, 3, 2, 7, 6, 5, 4]


def solution(mesh):
    f32 = jnp.float32
    col = pltpu.VMEM((NC, 8, 128), f32)
    fine = pltpu.VMEM((8, 8, 128), f32)
    row = pltpu.VMEM((1, 128), f32)
    scratch = [
        pltpu.VMEM((len(NAMES), 8, 128), f32), pltpu.VMEM((64, 128), f32),
        pltpu.VMEM((2, 128), f32), pltpu.VMEM((NC, 2, 128), f32),
        pltpu.VMEM((ROUNDS, 2, 8, 128), f32), pltpu.VMEM((ROUNDS, 2, 8, 128), f32), pltpu.VMEM((ROUNDS, 4, 1, 128), f32),
        pltpu.VMEM((ROUNDS, 2, 8, 128), f32), pltpu.VMEM((ROUNDS, 2, 8, 128), f32), pltpu.VMEM((ROUNDS, 4, 1, 128), f32),
        fine, fine, fine, fine, fine, fine,
        pltpu.VMEM((2, 8, 128), f32), pltpu.VMEM((2, NC, 8, 128), f32),
        col, col, col, col, col, col, col, col, col, col, col, col, pltpu.VMEM((NY, 8, 128), f32),
        row, pltpu.VMEM((32, 1, 128), f32), row, pltpu.VMEM((32, 1, 128), f32),
        pltpu.SemaphoreType.DMA, pltpu.SemaphoreType.DMA, pltpu.SemaphoreType.DMA,
        pltpu.SemaphoreType.DMA((ROUNDS, 8)), pltpu.SemaphoreType.DMA((ROUNDS, 8)),
        pltpu.SemaphoreType.DMA((2,)), pltpu.SemaphoreType.DMA((2,)),
        pltpu.SemaphoreType.DMA, pltpu.SemaphoreType.DMA, pltpu.SemaphoreType.DMA, pltpu.SemaphoreType.DMA,
        pltpu.SemaphoreType.REGULAR((4,)),
    ]
    vm = pl.BlockSpec(memory_space=pltpu.VMEM)
    call = pl.pallas_call(
        kernel,
        out_shape=[jax.ShapeDtypeStruct((8, 8, 128), f32), jax.ShapeDtypeStruct((8, 8, 128), f32), jax.ShapeDtypeStruct((1, 128), f32)],
        in_specs=[pl.BlockSpec(memory_space=pl.ANY), vm, vm, vm, vm],
        out_specs=[vm, vm, vm],
        scratch_shapes=scratch,
        compiler_params=pltpu.CompilerParams(collective_id=0, has_side_effects=True),
        name="helmholtz",
    )
    hot = (np.arange(128)[None, :] // 8 == np.arange(16)[:, None]).astype(np.float32)

    def local(forcing, kappa, sigma):
        s, r, e = call(jnp.asarray(TABLE), forcing, kappa.reshape(1, 16), sigma.reshape(1, 16), jnp.asarray(hot))
        return s, r, e[0, 0]

    return jax.shard_map(local, mesh=mesh, in_specs=(P("gx", "gy", None),) * 3,
                         out_specs=(P("gx", "gy", None), P("gx", "gy", None), P()), check_vma=False)
```

```python
import contextlib

import jax
import jax.numpy as jnp
import numpy as np
from jax import lax
from jax.experimental import pallas as pl
from jax.experimental.pallas import tpu as pltpu
from jax.sharding import PartitionSpec as P


def legendre_table(points, order):
    columns = [points * 0.0 + 1.0, points]
    for degree in range(2, order + 1):
        columns.append(((2 * degree - 1) * points * columns[-1] - (degree - 1) * columns[-2]) / degree)
    return np.stack(columns, axis=1)

def lobatto(count):
    order = count - 1
    points = np.cos(np.pi * np.arange(count) / order)
    for sweep in range(60):
        table = legendre_table(points, order)
        points = points - (points * table[:, order] - table[:, order - 1]) / (count * table[:, order])
    table = legendre_table(points, order)
    weights = 2.0 / (order * count * table[:, order] ** 2)
    values = table[:, order]
    points, weights, values = (points[::-1], weights[::-1], values[::-1])
    spread = points[:, None] - points[None, :] + np.eye(count)
    deriv = values[:, None] / values[None, :] / spread * (1.0 - np.eye(count))
    corner = order * (order + 1) / 4.0
    ends = np.array([-corner] + [0.0] * (count - 2) + [corner])
    return (points, weights, deriv + np.eye(count) * ends[None, :])

def lagrange(fine_points, coarse_points):
    columns = []
    for column in range(len(coarse_points)):
        value = fine_points * 0.0 + 1.0
        for other in range(len(coarse_points)):
            if other != column:
                value = value * (fine_points - coarse_points[other]) / (coarse_points[column] - coarse_points[other])
        columns.append(value)
    return np.stack(columns, axis=1)

X8, w8, D8 = lobatto(8); X4, w4, D4 = lobatto(4); X2, w2, D2 = lobatto(2)
J1 = lagrange(X8, X4)
J2 = lagrange(X4, X2)
K8, K4, K2 = (D.T @ (w[:, None] * D) for D, w in ((D8, w8), (D4, w4), (D2, w2)))
Kd8, Kd4, Kd2 = (np.diag(K) for K in (K8, K4, K2))
f8 = np.array([.5] + [1.]*6 + [.5]); f4 = np.array([.5, 1, 1, .5])
lane = np.arange(128)[None, :]; sub = np.arange(8)[:, None]
ones = np.ones((8, 128))
T = {}
def put(name, a): T[name] = np.ascontiguousarray(np.broadcast_to(a, (8, 128)).astype(np.float32))
kz = lane % 8
K8s = K8 / w8[:, None]
for d in range(1, 8):
    put(f"cy{d}", K8s[sub, (sub - d) % 8] * ones)
for d in range(-7, 8):
    if d == 0: continue
    src = kz - d; ok = (src >= 0) & (src < 8)
    put(f"cz{d}", np.where(ok, K8s[kz, np.clip(src, 0, 7)], 0.0))
put("cyz0", K8s[sub, sub] + K8s[kz, kz])
put("wyz", w8[sub] * w8[kz])
put("mz0", (kz == 0) * 1.0); put("mz7", (kz == 7) * 1.0)
put("jm0", (sub == 0) * 1.0); put("jm7", (sub == 7) * 1.0)
for i in range(4):
    put(f"gk{i}", (Kd8[i] * w8[sub] + w8[i] * Kd8[sub]) * w8[kz] + w8[i] * w8[sub] * Kd8[kz])
    put(f"gw{i}", w8[i] * w8[sub] * w8[kz])
put("m8", f8[sub] * f8[kz])
i4 = sub // 2; jp = sub % 2; h = lane % 2; k4 = (lane % 8) // 2; j4 = 2 * jp + h
for j in range(8):
    for hh in range(2):
        put(f"ry{j}_{hh}", J1[j, 2 * jp + hh] * ones)
RZ = []
for hh in range(2):
    for d in range(-7, 8):
        src = (lane % 8) - d; ok = (src >= 0) & (src < 8) & (h == hh)
        c = np.where(ok, J1[np.clip(src, 0, 7), k4], 0.0)
        if np.any(c != 0): put(f"rz{hh}_{d}", c); RZ.append((hh, d))
PZ = {}
for d in range(-7, 8):
    for hh in range(2):
        src = kz - d; ok = (src >= 0) & (src < 8) & (src % 2 == hh)
        c = np.where(ok, J1[kz, np.clip(src // 2, 0, 3)], 0.0)
        if np.any(c != 0): put(f"pz{hh}_{d}", c); PZ.setdefault(d, []).append(hh)
for b in range(4): put(f"py{b}", J1[sub, b] * ones)
def ops4(tag, M, dirs):
    M = np.asarray(M)
    if "x" in dirs:
        for d in range(4): put(f"{tag}x{d}", M[i4, (i4 - d) % 4] * ones)
    if "y" in dirs:
        put(f"{tag}ya", M[j4, j4]); put(f"{tag}yb", M[j4, 2 * (1 - jp) + h])
        put(f"{tag}yc", M[2 * jp + 1 - h, j4]); put(f"{tag}yd", M[2 * jp + 1 - h, 2 * (1 - jp) + h])
    if "z" in dirs:
        for d in range(-3, 4):
            src = k4 - d; ok = (src >= 0) & (src < 4)
            put(f"{tag}z{d}", np.where(ok, M[k4, np.clip(src, 0, 3)], 0.0))
K4s = K4 / w4[:, None]
for t in ("x", "y", "z"): ops4("a", K4s, t)
put("a0", K4s[i4, i4] + K4s[j4, j4] + K4s[k4, k4])
put("W1", w4[i4] * w4[j4] * w4[k4])
put("G1", Kd4[i4] * w4[j4] * w4[k4] + w4[i4] * Kd4[j4] * w4[k4] + w4[i4] * w4[j4] * Kd4[k4])
put("m1", f4[i4] * f4[j4] * f4[k4])
put("z0", (k4 == 0) * 1.0); put("z3", (k4 == 3) * 1.0)
put("x0", (i4 == 0) * 1.0); put("x3", (i4 == 3) * 1.0)
put("y0", (j4 == 0) * 1.0); put("y3", (j4 == 3) * 1.0)
cor = lambda a: (a == 0) | (a == 3)
cmask = (cor(i4) & cor(j4) & cor(k4)) * 1.0
R2 = np.zeros((4, 4)); R2[0] = J2[:, 0]; R2[3] = J2[:, 1]
P2 = np.zeros((4, 4)); P2[:, 0] = J2[:, 0]; P2[:, 3] = J2[:, 1]
K2s = K2 / w2[:, None]
B2 = np.zeros((4, 4)); B2[np.ix_([0, 3], [0, 3])] = K2s
for t in ("x", "y", "z"):
    ops4("r", R2, t); ops4("p", P2, t); ops4("b", B2, t)
w2e = np.array([w2[0], 0, 0, w2[1]]); Kd2e = np.array([Kd2[0], 0, 0, Kd2[1]])
put("W2", w2e[i4] * w2e[j4] * w2e[k4])
put("G2", Kd2e[i4] * w2e[j4] * w2e[k4] + w2e[i4] * Kd2e[j4] * w2e[k4] + w2e[i4] * w2e[j4] * Kd2e[k4])
put("off2", 1.0 - cmask)
KJ = K8s @ J1
KJx = K8 @ J1
for d in range(-7, 8):
    for hh in range(2):
        src = kz - d; ok = (src >= 0) & (src < 8) & (src % 2 == hh)
        put(f"qz{hh}_{d}", np.where(ok, KJ[kz, np.clip(src // 2, 0, 3)], 0.0))
for b in range(4): put(f"qy{b}", KJ[sub, b] * ones)
for j0 in (0, 7):
    for hh in range(2): put(f"fy{j0}_{hh}", KJ[j0, 2 * jp + hh] * ones)
for i0 in (0, 7):
    for j0 in (0, 7):
        a0, b0 = (0 if i0 == 0 else 3), (0 if j0 == 0 else 3)
        for hh in range(2):
            b_ = 2 * jp + hh
            put(f"fc{i0}{j0}_{hh}", (KJ[i0, i4] * (b_ == b0) + KJ[j0, b_] * (i4 == a0)) * ones)
        put(f"fo{i0}{j0}", ((i4 == a0) & (jp == b0 // 2)) * ones)
for q in range(2): put(f"hot{q}", (lane // 8 == sub + 8 * q) * 1.0)
NZ_ = lambda n: np.any(T[n] != 0)
THETA, DELTA = 1.65, 1.35
S_ = THETA / DELTA; rho0 = 1 / S_; rho1 = 1 / (2 * S_ - rho0)
ALPHA = rho1 * rho0; BETA = 2 * rho1 / DELTA

NAMES = [n for n in T if np.any(T[n])]
INDEX = {n: k for k, n in enumerate(NAMES)}
TABLE = np.stack([T[n] for n in NAMES])
K8 = [[float(np.float32(x)) for x in r] for r in K8]
w8 = [float(np.float32(x)) for x in w8]


def live(name):
    return name in INDEX


def lr(v, s):
    return pltpu.roll(v, s % 128, 1)


def sr(v, s):
    return pltpu.roll(v, s % 8, 0)


def halves():
    s = lax.broadcasted_iota(jnp.int32, (8, 128), 0)
    l = lax.broadcasted_iota(jnp.int32, (8, 128), 1)
    return s % 2 == 1, l % 2 == 1

def zops(C, tag, v, skip0=False):
    out = None
    for d in range(-3, 4):
        if (d == 0 and skip0) or not live(f"{tag}z{d}"): continue
        t = C(f"{tag}z{d}") * (lr(v, 2 * d) if d else v)
        out = t if out is None else out + t
    return out

def xops(C, tag, v, skip0=False):
    out = None
    for d in range(4):
        if (d == 0 and skip0) or not live(f"{tag}x{d}"): continue
        t = C(f"{tag}x{d}") * (sr(v, 2 * d) if d else v)
        out = t if out is None else out + t
    return out

def yops(C, tag, v, skip0=False):
    jp1, h1 = halves()
    sw = jnp.where(jp1, sr(v, 1), sr(v, -1)) if live(f"{tag}yb") or live(f"{tag}yd") else None
    def pair(a, b):
        t = None
        if live(a): t = C(a) * v
        if live(b): t = C(b) * sw if t is None else t + C(b) * sw
        return t
    other = pair(f"{tag}yc", f"{tag}yd")
    out = None if other is None else jnp.where(h1, lr(other, 1), lr(other, -1))
    if skip0:
        if live(f"{tag}yb"): out = out + C(f"{tag}yb") * sw
        return out
    same = pair(f"{tag}ya", f"{tag}yb")
    return same if out is None else (out if same is None else out + same)

def a1(C, v, kap, sig):
    k = C("a0") * v + xops(C, "a", v, True) + yops(C, "a", v, True) + zops(C, "a", v, True)
    return C("W1") * (kap * k + sig * v)

def a2(C, v, kap, sig):
    k = xops(C, "b", v) + yops(C, "b", v) + zops(C, "b", v)
    return C("W2") * (kap * k + sig * v)

def restrict2(C, v): return zops(C, "r", yops(C, "r", xops(C, "r", v)))
def prolong2(C, v): return xops(C, "p", yops(C, "p", zops(C, "p", v)))
def sz1(C, v): return v + C("z0") * lr(v, 2) + C("z3") * lr(v, -2)
def xfrom_l(C, v): return C("x0") * sr(v, 2)
def xfrom_r(C, v): return C("x3") * sr(v, -2)
def yfrom_l(C, v): return C("y0") * lr(sr(v, -1), -1)
def yfrom_r(C, v): return C("y3") * lr(sr(v, 1), 1)

def a_fine(C, v, c1, rho):
    e = C("cyz0") + rho
    out = []
    for i in range(8):
        t = e * v[i]
        for d in range(1, 8): t = t + C(f"cy{d}") * sr(v[i], d)
        for d in range(-7, 8):
            if d: t = t + C(f"cz{d}") * lr(v[i], d)
        x = K8[i][0] * v[0]
        for a in range(1, 8): x = x + K8[i][a] * v[a]
        out.append(c1 * (x + w8[i] * t))
    return out

def sz8(C, v): return v + C("mz0") * lr(v, 1) + C("mz7") * lr(v, -1)


def scope(name):
    return contextlib.nullcontext()


MESH = pl.DeviceIdType.MESH
NY = 4
ZR = 32
YR = 4
GX = ZR * YR * 2
R = 6
NC = (2 * R + 1) * NY
OWN = R * NY
PARTNERS = [(dx, dy) for dx in range(-R, R + 1) for dy in range(NY) if (dx, dy) != (0, 0)]
ROUNDS = 7
TI = 1.0 / THETA


def slot(dx, dy):
    return (dx + R) * NY + dy % NY


def kernel(tab_hbm, forc_hbm, kap_hbm, sig_hbm, z_out, b_out, r_out, scal,
           tab, forc, kap_in, sig_in, V, ks_s, KS, SX, SY, SC, RX, RY, RC, ID0, B, D0, R1, Q, XS,
           us, U, ID1, ID2, C1B, D0B, VA, R1B, D1B, VB, C2B, G0B, QB, VC, X1, TMP, Z,
           ap, AZ, pp, AP,
           in_sem, out_sem, ks_send, kf_send, kf_recv, ks_recv, f_send, f_recv, u_send, u_recv,
           z_send, z_recv, p_send, p_recv, chain):
    gx = lax.axis_index("gx")
    gy = lax.axis_index("gy")
    core = lax.rem(gx, 2)
    zc = lax.rem(gx // 2, ZR)
    yc = gx // (2 * ZR)

    def at(dx, dy):
        return (lax.rem(gx + dx + GX, GX), lax.rem(gy + dy + NY, NY))

    def zring(k):
        return (yc * (2 * ZR) + 2 * lax.rem(zc + k + ZR, ZR) + core, gy)

    def plane(dy, dc, dx):
        return (lax.rem(yc + dy, YR) * (2 * ZR) + 2 * zc + lax.rem(core + dc, 2), lax.rem(gy + dx, NY))

    def C(name):
        return tab[INDEX[name]]

    loads = [pltpu.make_async_copy(a, b, in_sem.at[k]) for k, (a, b) in enumerate(((kap_hbm, kap_in), (sig_hbm, sig_in), (tab_hbm, tab), (forc_hbm, forc)))]
    for c in loads:
        c.start()
    barrier = pltpu.get_barrier_semaphore()
    greet = [at(dx, dy) for dx, dy in PARTNERS]
    greet += [zring(k) for k in (-3, -2, -1, 1, 2, 3)] + [plane(k, 0, 0) for k in (1, 2, 3)]
    for d in greet:
        pl.semaphore_signal(barrier, inc=1, device_id=d, device_id_type=MESH)

    with scope('tab_wait'):
        for c in loads:
            c.wait()
    hot = jnp.concatenate([C("hot0"), C("hot1")], axis=0)
    def lanes(ref):
        return jnp.dot(jnp.broadcast_to(ref[...], (8, 16)), hot, precision=lax.Precision.HIGHEST, preferred_element_type=jnp.float32)
    kap = lanes(kap_in)
    sig = lanes(sig_in)
    ks_s[0:1] = kap[0:1]
    ks_s[1:2] = sig[0:1]
    KS[OWN, 0:1] = kap[0:1]
    KS[OWN, 1:2] = sig[0:1]

    def put_faces(rnd):
        SX[rnd, 0] = V[0:8]
        SX[rnd, 1] = V[56:64]
        SY[rnd, 0] = V[pl.ds(0, 8, stride=8)]
        SY[rnd, 1] = V[pl.ds(7, 8, stride=8)]
        for k, row in enumerate((0, 7, 56, 63)):
            SC[rnd, k] = V[row:row + 1]

    def face_copies(rnd):
        out = []
        for s in range(2):
            step = 2 * s - 1
            out.append((SX.at[rnd, s], RX.at[rnd, 1 - s], at(step, 0)))
        for s in range(2):
            step = 2 * s - 1
            out.append((SY.at[rnd, s], RY.at[rnd, 1 - s], at(0, step)))
        for k in range(4):
            out.append((SC.at[rnd, k], RC.at[rnd, 3 - k], at(2 * (k // 2) - 1, 2 * (k % 2) - 1)))
        return [pltpu.make_async_remote_copy(src_ref=a, dst_ref=b, send_sem=f_send.at[rnd, n], recv_sem=f_recv.at[rnd, RSEM[n]],
                                             device_id=d, device_id_type=MESH) for n, (a, b, d) in enumerate(out)]

    def face_start(rnd, tiles):
        for i in range(8):
            V[8 * i:8 * i + 8] = tiles[i]
        put_faces(rnd)
        with scope('face_start'):
            for c in face_copies(rnd):
                c.start()

    def face_wait(rnd):
        with scope('face_wait'):
            for n in range(8):
                pltpu.make_async_remote_copy(src_ref=(RX.at[rnd, n] if n < 2 else RY.at[rnd, n - 2] if n < 4 else RC.at[rnd, n - 4]),
                                             dst_ref=(RX.at[rnd, n] if n < 2 else RY.at[rnd, n - 2] if n < 4 else RC.at[rnd, n - 4]),
                                             send_sem=f_send.at[rnd, n], recv_sem=f_recv.at[rnd, n], device_id=at(1, 0), device_id_type=MESH).wait_recv()
        V[0:8] = V[0:8] + RX[rnd, 0]
        V[56:64] = V[56:64] + RX[rnd, 1]
        V[pl.ds(0, 8, stride=8)] = V[pl.ds(0, 8, stride=8)] + RY[rnd, 0]
        V[pl.ds(7, 8, stride=8)] = V[pl.ds(7, 8, stride=8)] + RY[rnd, 1]
        for k, row in enumerate((0, 7, 56, 63)):
            V[row:row + 1] = V[row:row + 1] + RC[rnd, k]
        return [V[8 * i:8 * i + 8] for i in range(8)]

    first_v = [sz8(C, forc[i]) for i in range(8)]
    with scope('barrier'):
        pl.semaphore_wait(barrier, len(greet))

    def ks_copy(dx, dy):
        near = abs(dx) <= 1 and dy != 2
        return pltpu.make_async_remote_copy(src_ref=ks_s, dst_ref=KS.at[slot(-dx, -dy)], send_sem=ks_send if near else kf_send,
                                            recv_sem=ks_recv if near else kf_recv, device_id=at(dx, dy), device_id_type=MESH)
    near = [(dx, dy) for dx, dy in PARTNERS if abs(dx) <= 1 and dy != 2]
    far = [p for p in PARTNERS if p not in near]
    for p in near:
        ks_copy(*p).start()
    face_start(0, first_v)
    with scope('ks_send'):
        for p in far:
            ks_copy(*p).start()
    for k in (-3, 3):
        pl.semaphore_signal(chain.at[0], inc=1, device_id=zring(k), device_id_type=MESH)
    for k in (1, 2, 3):
        pl.semaphore_signal(chain.at[3], inc=1, device_id=plane(k, 0, 0), device_id_type=MESH)

    def landed(buf, count, send, recv):
        return pltpu.make_async_remote_copy(src_ref=buf.at[pl.ds(0, count)], dst_ref=buf.at[pl.ds(0, count)], send_sem=send, recv_sem=recv,
                                            device_id=at(1, 0), device_id_type=MESH)

    with scope('ks_wait'):
        landed(KS, len(near), ks_send, ks_recv).wait_recv()

    def row(dx, dy, which):
        return KS[slot(dx, dy), which:which + 1]
    prof = [[], []]
    for dx in (-1, 0, 1):
        for which in range(2):
            prof[which].append(row(dx, 0, which) + C("jm0") * row(dx, -1, which) + C("jm7") * row(dx, 1, which))
    for i in range(8):
        kk, ss = prof[0][1], prof[1][1]
        if i == 0:
            kk, ss = kk + prof[0][0], ss + prof[1][0]
        if i == 7:
            kk, ss = kk + prof[0][2], ss + prof[1][2]
        ii = min(i, 7 - i)
        ID0[i] = 1.0 / sz8(C, kk * C(f"gk{ii}") + ss * C(f"gw{ii}"))

    b = face_wait(0)
    for i in range(8):
        B[i] = b[i]
        R1[i] = b[i]
        XS[i] = jnp.zeros((8, 128), jnp.float32)

    def kap_of(dx, dy):
        return KS[(dx + R) * NY + dy, 0:1]

    def sig_of(dx, dy):
        return KS[(dx + R) * NY + dy, 1:2]

    def assembled(buf, dx):
        base = (dx + R) * NY
        u = [buf[base + dy] + xfrom_l(C, buf[base - NY + dy]) + xfrom_r(C, buf[base + NY + dy]) for dy in range(NY)]
        up = [yfrom_l(C, u[dy]) for dy in range(NY)]
        dn = [yfrom_r(C, u[dy]) for dy in range(NY)]
        return [u[dy] + up[(dy - 1) % NY] + dn[(dy + 1) % NY] for dy in range(NY)]

    def over(radius, body):
        for dx in range(-radius, radius + 1):
            body(dx)

    def coarse_diagonals():
        with scope('kf_wait'):
            landed(KS, len(far), kf_send, kf_recv).wait_recv()
        def g_one(dx):
            for dy in range(NY):
                c = (dx + R) * NY + dy
                VA[c] = sz1(C, kap_of(dx, dy) * C("G1") + sig_of(dx, dy) * C("W1"))
                VB[c] = sz1(C, kap_of(dx, dy) * C("G2") + sig_of(dx, dy) * C("W2"))
        with scope('g_one'):
            over(R, g_one)
        def g_two(dx):
            s1, s2 = assembled(VA, dx), assembled(VB, dx)
            for dy in range(NY):
                c = (dx + R) * NY + dy
                ID1[c] = 1.0 / s1[dy]
                ID2[c] = 1.0 / (s2[dy] + C("off2"))
        with scope('g_two'):
            over(R - 1, g_two)

    pl.semaphore_wait(chain.at[0], 2)
    for k in (-6, 6):
        pl.semaphore_signal(chain.at[1], inc=1, device_id=zring(k), device_id_type=MESH)

    c1 = kap * C("wyz")
    rho = sig / kap

    def tiles(ref):
        return [ref[i] for i in range(8)]

    def u_copy(cyc, dx, dy):
        return pltpu.make_async_remote_copy(src_ref=us.at[cyc], dst_ref=U.at[cyc, slot(-dx, -dy)], send_sem=u_send.at[cyc], recv_sem=u_recv.at[cyc],
                                            device_id=at(dx, dy), device_id_type=MESH)

    def columns(radius):
        return [(dx, dy, (dx + R) * NY + dy) for dx in range(-radius, radius + 1) for dy in range(NY)]

    def sums(buf, radius, put):
        for dx in range(-radius, radius + 1):
            s = assembled(buf, dx)
            for dy in range(NY):
                put((dx + R) * NY + dy, s[dy])

    def image(op, src, dst, radius):
        for dx, dy, c in columns(radius):
            TMP[c] = op(C, src[c], kap_of(dx, dy), sig_of(dx, dy))
        for dx, dy, c in columns(radius):
            dst[c] = sz1(C, TMP[c])

    def coarse(cyc):
        def put1(c, s):
            C1B[c] = s
            D0B[c] = TI * s * ID1[c]
        def put2(c, s):
            r1 = C1B[c] - s
            R1B[c] = r1
            D1B[c] = ALPHA * D0B[c] + BETA * r1 * ID1[c]
        def put3(c, s):
            C2B[c] = s
            G0B[c] = TI * s * ID2[c]
        def put4(c, s):
            QB[c] = (1.0 + ALPHA) * G0B[c] + BETA * (C2B[c] - s) * ID2[c]
        with scope('first'):
            sums(U.at[cyc], R - 1, put1)
            image(a1, D0B, VA, R - 1)
        with scope('second'):
            sums(VA, R - 2, put2)
            for dx, dy, c in columns(R - 2):
                TMP[c] = C("m1") * R1B[c] - a1(C, D1B[c], kap_of(dx, dy), sig_of(dx, dy))
            for dx, dy, c in columns(R - 2):
                TMP[c] = yops(C, "r", xops(C, "r", TMP[c]))
            for dx, dy, c in columns(R - 2):
                TMP[c] = zops(C, "r", TMP[c])
            for dx, dy, c in columns(R - 2):
                VB[c] = sz1(C, TMP[c])
        with scope('third'):
            sums(VB, R - 3, put3)
            image(a2, G0B, VA, R - 3)
        with scope('fourth'):
            sums(VA, R - 4, put4)
            for dx, dy, c in columns(R - 4):
                TMP[c] = zops(C, "p", QB[c])
            for dx, dy, c in columns(R - 4):
                QB[c] = D1B[c] + xops(C, "p", yops(C, "p", TMP[c]))
            image(a1, QB, VC, R - 4)
        with scope('fifth'):
            def put5(c, s):
                X1[c] = D0B[c] + QB[c] + TI * (R1B[c] - s) * ID1[c]
            sums(VC, R - 5, put5)

    def restrict1(t):
        xs = [sum(float(J1[i, a]) * t[i] for i in range(8)) for a in range(4)]
        for s in range(8):
            V[8 * s:8 * s + 8] = xs[s // 2]
        out = None
        for hh in range(2):
            y = None
            for j in range(8):
                if live(f"ry{j}_{hh}"):
                    p = C(f"ry{j}_{hh}") * V[pl.ds(j, 8, stride=8)]
                    y = p if y is None else y + p
            for h2, d in RZ:
                if h2 == hh:
                    p = C(f"rz{hh}_{d}") * (lr(y, d) if d else y)
                    out = p if out is None else out + p
        return out

    around = [(dx, dy) for dx in (-1, 0, 1) for dy in (-1, 0, 1)]

    def lines():
        for n, (dx, dy) in enumerate(around):
            e = X1[slot(dx, dy)]
            z = [None] * 4
            for d in range(-7, 8):
                r = lr(e, d) if d else e
                for hh in range(2):
                    for q, tag in enumerate(("pz", "qz")):
                        if not live(f"{tag}{hh}_{d}"):
                            continue
                        p = C(f"{tag}{hh}_{d}") * r
                        z[2 * q + hh] = p if z[2 * q + hh] is None else z[2 * q + hh] + p
            for q in range(4):
                Z[n, 8 * q:8 * q + 8] = z[q]

    def line(n, q, a, b):
        return Z[n, pl.ds(16 * q + 8 * (b % 2) + 2 * a + b // 2, 8, stride=0)]

    def planes(n, a):
        return sum(C(f"py{b}") * line(n, 0, a, b) for b in range(4))

    def planes_image(n, a, rho_n, ex):
        return sum(C(f"qy{b}") * line(n, 0, a, b) + C(f"py{b}") * line(n, 1, a, b) for b in range(4)) + rho_n * ex

    def correction():
        lines()
        rhos = [row(dx, dy, 1) / row(dx, dy, 0) for dx, dy in around]
        ex = [planes(4, a) for a in range(4)]
        ey = [planes_image(4, a, rho, ex[a]) for a in range(4)]
        e = [sum(float(J1[i, a]) * ex[a] for a in range(4)) for i in range(8)]
        for i in range(8):
            V[8 * i:8 * i + 8] = c1 * (sum(float(KJx[i, a]) * ex[a] for a in range(4)) + w8[i] * sum(float(J1[i, a]) * ey[a] for a in range(4)))
        for n, (dx, dy) in enumerate(around):
            kap_n, rho_n = row(dx, dy, 0), rhos[n]
            i0, j0 = (7 if dx < 0 else 0), (7 if dy < 0 else 0)
            a0, b0 = (3 if dx < 0 else 0), (3 if dy < 0 else 0)
            if dx and dy:
                t = C(f"fc{i0}{j0}_0") * Z[n, 0:8] + C(f"fc{i0}{j0}_1") * Z[n, 8:16]
                hh = b0 % 2
                t = t + C(f"fo{i0}{j0}") * (Z[n, 16 + 8 * hh:24 + 8 * hh] + rho_n * Z[n, 8 * hh:8 * hh + 8])
                t = t + sr(t, 4)
                t = t + sr(t, 2)
                t = t + sr(t, 1)
                r = 8 * (7 - i0) + 7 - j0
                V[r:r + 1] = V[r:r + 1] + (kap_n * (w8[i0] * C("wyz")[0:1] * (w8[j0] / w8[0]))) * t[0:1]
            elif dx:
                q = [planes(n, a) for a in range(4)]
                t = sum(float(KJx[i0, a]) * q[a] for a in range(4)) + w8[i0] * planes_image(n, a0, rho_n, q[a0])
                r = 8 * (7 - i0)
                V[r:r + 8] = V[r:r + 8] + (kap_n * C("wyz")) * t
            elif dy:
                t = C(f"fy{j0}_0") * Z[n, 0:8] + C(f"fy{j0}_1") * Z[n, 8:16]
                t = t + jnp.where(halves()[0], sr(t, 1), sr(t, -1))
                hh = b0 % 2
                t = t + Z[n, 16 + 8 * hh:24 + 8 * hh] + rho_n * Z[n, 8 * hh:8 * hh + 8]
                Z[n, 32:40] = t
                f = sum(C(f"py{a}") * Z[n, pl.ds(32 + 2 * a + b0 // 2, 8, stride=0)] + C(f"qy{a}") * line(n, 0, a, b0) for a in range(4))
                V[pl.ds(7 - j0, 8, stride=8)] = V[pl.ds(7 - j0, 8, stride=8)] + (kap_n * C("wyz") * w8[j0]) * f
        return e

    def apply(rnd, v):
        face_start(rnd, [sz8(C, t) for t in a_fine(C, v, c1, rho)])
        return face_wait(rnd)

    def cycle(cyc, carry):
        rnd = 1 + 3 * cyc
        r = tiles(R1)
        d0 = [TI * r[i] * ID0[i] for i in range(8)]
        for i in range(8):
            D0[i] = d0[i]
        s = apply(rnd, d0)
        d1, t = [], []
        for i in range(8):
            r1 = R1[i] - s[i]
            R1[i] = r1
            d1.append(ALPHA * D0[i] + BETA * r1 * ID0[i])
            Q[i] = d1[i]
        w = a_fine(C, d1, c1, rho)
        t = [float(f8[i]) * C("m8") * R1[i] - w[i] for i in range(8)]
        u = sz1(C, restrict1(t))
        us[cyc] = u
        U[cyc, OWN] = u
        with scope('u_send'):
            for dx, dy in PARTNERS:
                u_copy(cyc, dx, dy).start()
        face_start(rnd + 1, [sz8(C, p) for p in w])
        @pl.when(cyc == 0)
        def _():
            coarse_diagonals()
            pl.semaphore_wait(chain.at[1], 2)
            for k in (-10, 10):
                pl.semaphore_signal(chain.at[2], inc=1, device_id=zring(k), device_id_type=MESH)
        s = face_wait(rnd + 1)
        for i in range(8):
            R1[i] = R1[i] - s[i]
        with scope('u_wait'):
            landed(U.at[cyc], NC - 1, u_send.at[cyc], u_recv.at[cyc]).wait_recv()
        coarse(cyc)
        with scope('corr'):
            e = correction()
        for i in range(8):
            Q[i] = Q[i] + e[i]
        s = [sz8(C, V[8 * i:8 * i + 8]) for i in range(8)]
        dl = []
        for i in range(8):
            r3 = R1[i] - s[i]
            R1[i] = r3
            x = TI * r3 * ID0[i]
            dl.append(x)
            XS[i] = XS[i] + (D0[i] + Q[i] + x)
        s = apply(rnd + 2, dl)
        for i in range(8):
            R1[i] = R1[i] - s[i]
        return carry

    lax.fori_loop(0, 2, cycle, 0)

    def dot(p, q):
        t = sum(float(f8[i]) * C("m8") * p[i] * q[i] for i in range(8))
        return jnp.sum(jnp.sum(t, axis=1, keepdims=True), axis=0, keepdims=True)
    ln = lax.broadcasted_iota(jnp.int32, (1, 128), 1)
    mine = jnp.where(ln == 0, dot(B, B), jnp.where(ln == 1, dot(B, R1), dot(R1, R1)))
    ap[...] = mine
    AZ[zc] = mine
    pl.semaphore_wait(chain.at[2], 2)
    pl.semaphore_wait(chain.at[3], 3)
    def z_copy(k):
        return pltpu.make_async_remote_copy(src_ref=ap, dst_ref=AZ.at[zc], send_sem=z_send, recv_sem=z_recv, device_id=zring(k), device_id_type=MESH)
    with scope('z_send'):
        for k in range(1, ZR // 2):
            z_copy(k).start()
            z_copy(-k).start()
        z_copy(ZR // 2).start()
    stores = [pltpu.make_async_copy(a, b, out_sem.at[k]) for k, (a, b) in enumerate(((XS, z_out), (B, b_out), (R1, r_out)))]
    for c in stores:
        c.start()
    def most(buf, send, recv):
        return pltpu.make_async_remote_copy(src_ref=buf.at[pl.ds(0, 31)], dst_ref=buf.at[pl.ds(0, 31)], send_sem=send, recv_sem=recv,
                                            device_id=at(1, 0), device_id_type=MESH)
    with scope('z_wait'):
        most(AZ, z_send, z_recv).wait_recv()
    part = AZ[0]
    for k in range(1, ZR):
        part = part + AZ[k]
    pp[...] = part
    pi = yc * 8 + gy * 2 + core
    AP[pi] = part
    others = [(a, c, x) for a in range(YR) for c in range(2) for x in range(NY) if (a, c, x) != (0, 0, 0)]
    def p_copy(o):
        return pltpu.make_async_remote_copy(src_ref=pp, dst_ref=AP.at[pi], send_sem=p_send, recv_sem=p_recv, device_id=plane(*o), device_id_type=MESH)
    for o in others:
        p_copy(o).start()
    with scope('p_wait'):
        most(AP, p_send, p_recv).wait_recv()
    tot = AP[0]
    for k in range(1, 32):
        tot = tot + AP[k]
    bb, br, rr = tot[0:1, 0:1], tot[0:1, 1:2], tot[0:1, 2:3]
    ww = bb - 2.0 * br + rr
    coef = (bb - br) / ww
    size = jnp.sqrt((bb * rr - br * br) / (ww * bb))
    scal[...] = jnp.where(ln == 0, coef, size)
    for c in stores:
        c.wait()

    with scope('send_waits'):
        most(AP, p_send, p_recv).wait_send()
    most(AZ, z_send, z_recv).wait_send()
    landed(KS, len(near), ks_send, ks_recv).wait_send()
    landed(KS, len(far), kf_send, kf_recv).wait_send()
    for cyc in range(2):
        landed(U.at[cyc], NC - 1, u_send.at[cyc], u_recv.at[cyc]).wait_send()
    for rnd in range(ROUNDS):
        for c in face_copies(rnd):
            c.wait_send()


RSEM = [1, 0, 3, 2, 7, 6, 5, 4]


def solution(mesh):
    f32 = jnp.float32
    col = pltpu.VMEM((NC, 8, 128), f32)
    fine = pltpu.VMEM((8, 8, 128), f32)
    row = pltpu.VMEM((1, 128), f32)
    scratch = [
        pltpu.VMEM((len(NAMES), 8, 128), f32), fine, pltpu.VMEM((1, 16), f32), pltpu.VMEM((1, 16), f32), pltpu.VMEM((64, 128), f32),
        pltpu.VMEM((2, 128), f32), pltpu.VMEM((NC, 2, 128), f32),
        pltpu.VMEM((ROUNDS, 2, 8, 128), f32), pltpu.VMEM((ROUNDS, 2, 8, 128), f32), pltpu.VMEM((ROUNDS, 4, 1, 128), f32),
        pltpu.VMEM((ROUNDS, 2, 8, 128), f32), pltpu.VMEM((ROUNDS, 2, 8, 128), f32), pltpu.VMEM((ROUNDS, 4, 1, 128), f32),
        fine, fine, fine, fine, fine, fine,
        pltpu.VMEM((2, 8, 128), f32), pltpu.VMEM((2, NC, 8, 128), f32),
        col, col, col, col, col, col, col, col, col, col, col, col, col, col, pltpu.VMEM((9, 40, 128), f32),
        row, pltpu.VMEM((32, 1, 128), f32), row, pltpu.VMEM((32, 1, 128), f32),
        pltpu.SemaphoreType.DMA((4,)), pltpu.SemaphoreType.DMA((3,)),
        pltpu.SemaphoreType.DMA, pltpu.SemaphoreType.DMA, pltpu.SemaphoreType.DMA, pltpu.SemaphoreType.DMA,
        pltpu.SemaphoreType.DMA((ROUNDS, 8)), pltpu.SemaphoreType.DMA((ROUNDS, 8)),
        pltpu.SemaphoreType.DMA((2,)), pltpu.SemaphoreType.DMA((2,)),
        pltpu.SemaphoreType.DMA, pltpu.SemaphoreType.DMA, pltpu.SemaphoreType.DMA, pltpu.SemaphoreType.DMA,
        pltpu.SemaphoreType.REGULAR((4,)),
    ]
    hbm = pl.BlockSpec(memory_space=pl.ANY)
    call = pl.pallas_call(
        kernel,
        out_shape=[jax.ShapeDtypeStruct((8, 8, 128), f32)] * 3 + [jax.ShapeDtypeStruct((1, 128), f32)],
        in_specs=[hbm] * 4,
        out_specs=[hbm] * 3 + [pl.BlockSpec(memory_space=pltpu.VMEM)],
        scratch_shapes=scratch,
        compiler_params=pltpu.CompilerParams(collective_id=0, has_side_effects=True),
        name="helmholtz",
    )
    def local(forcing, kappa, sigma):
        z, b, r, scal = call(jnp.asarray(TABLE), forcing, kappa.reshape(1, 16), sigma.reshape(1, 16))
        coef = scal[0, 0]
        return coef * z, b - coef * (b - r), scal[0, 1]

    return jax.shard_map(local, mesh=mesh, in_specs=(P("gx", "gy", None),) * 3,
                         out_specs=(P("gx", "gy", None), P("gx", "gy", None), P()), check_vma=False)
```

```python
import contextlib

import jax
import jax.numpy as jnp
import numpy as np
from jax import lax
from jax.experimental import pallas as pl
from jax.experimental.pallas import tpu as pltpu
from jax.sharding import PartitionSpec as P


def legendre_table(points, order):
    columns = [points * 0.0 + 1.0, points]
    for degree in range(2, order + 1):
        columns.append(((2 * degree - 1) * points * columns[-1] - (degree - 1) * columns[-2]) / degree)
    return np.stack(columns, axis=1)

def lobatto(count):
    order = count - 1
    points = np.cos(np.pi * np.arange(count) / order)
    for sweep in range(60):
        table = legendre_table(points, order)
        points = points - (points * table[:, order] - table[:, order - 1]) / (count * table[:, order])
    table = legendre_table(points, order)
    weights = 2.0 / (order * count * table[:, order] ** 2)
    values = table[:, order]
    points, weights, values = (points[::-1], weights[::-1], values[::-1])
    spread = points[:, None] - points[None, :] + np.eye(count)
    deriv = values[:, None] / values[None, :] / spread * (1.0 - np.eye(count))
    corner = order * (order + 1) / 4.0
    ends = np.array([-corner] + [0.0] * (count - 2) + [corner])
    return (points, weights, deriv + np.eye(count) * ends[None, :])

def lagrange(fine_points, coarse_points):
    columns = []
    for column in range(len(coarse_points)):
        value = fine_points * 0.0 + 1.0
        for other in range(len(coarse_points)):
            if other != column:
                value = value * (fine_points - coarse_points[other]) / (coarse_points[column] - coarse_points[other])
        columns.append(value)
    return np.stack(columns, axis=1)

X8, w8, D8 = lobatto(8); X4, w4, D4 = lobatto(4); X2, w2, D2 = lobatto(2)
J1 = lagrange(X8, X4)
J2 = lagrange(X4, X2)
K8, K4, K2 = (D.T @ (w[:, None] * D) for D, w in ((D8, w8), (D4, w4), (D2, w2)))
Kd8, Kd4, Kd2 = (np.diag(K) for K in (K8, K4, K2))
f8 = np.array([.5] + [1.]*6 + [.5]); f4 = np.array([.5, 1, 1, .5])
lane = np.arange(128)[None, :]; sub = np.arange(8)[:, None]
ones = np.ones((8, 128))
T = {}
def put(name, a): T[name] = np.ascontiguousarray(np.broadcast_to(a, (8, 128)).astype(np.float32))
kz = lane % 8
K8s = K8 / w8[:, None]
for d in range(1, 8):
    put(f"cy{d}", K8s[sub, (sub - d) % 8] * ones)
for d in range(-7, 8):
    if d == 0: continue
    src = kz - d; ok = (src >= 0) & (src < 8)
    put(f"cz{d}", np.where(ok, K8s[kz, np.clip(src, 0, 7)], 0.0))
put("cyz0", K8s[sub, sub] + K8s[kz, kz])
put("wyz", w8[sub] * w8[kz])
put("mz0", (kz == 0) * 1.0); put("mz7", (kz == 7) * 1.0)
put("jm0", (sub == 0) * 1.0); put("jm7", (sub == 7) * 1.0)
for i in range(4):
    put(f"gk{i}", (Kd8[i] * w8[sub] + w8[i] * Kd8[sub]) * w8[kz] + w8[i] * w8[sub] * Kd8[kz])
    put(f"gw{i}", w8[i] * w8[sub] * w8[kz])
put("m8", f8[sub] * f8[kz])
i4 = sub // 2; jp = sub % 2; h = lane % 2; k4 = (lane % 8) // 2; j4 = 2 * jp + (h ^ jp); jsw = 2 * (1 - jp) + (h ^ (1 - jp)); jot = 2 * jp + ((1 - h) ^ jp)
for j in range(8):
    for hh in range(2):
        put(f"ry{j}_{hh}", J1[j, 2 * jp + (hh ^ jp)] * ones)
RZ = []
for hh in range(2):
    for d in range(-7, 8):
        src = (lane % 8) - d; ok = (src >= 0) & (src < 8) & (h == hh)
        c = np.where(ok, J1[np.clip(src, 0, 7), k4], 0.0)
        if np.any(c != 0): put(f"rz{hh}_{d}", c); RZ.append((hh, d))
PZ = {}
for d in range(-7, 8):
    for hh in range(2):
        src = kz - d; ok = (src >= 0) & (src < 8) & (src % 2 == hh)
        c = np.where(ok, J1[kz, np.clip(src // 2, 0, 3)], 0.0)
        if np.any(c != 0): put(f"pz{hh}_{d}", c); PZ.setdefault(d, []).append(hh)
for b in range(4): put(f"py{b}", J1[sub, b] * ones)
def ops4(tag, M, dirs):
    M = np.asarray(M)
    if "x" in dirs:
        for d in range(4): put(f"{tag}x{d}", M[i4, (i4 - d) % 4] * ones)
    if "y" in dirs:
        put(f"{tag}ya", M[j4, j4]); put(f"{tag}yb", M[j4, jsw])
        put(f"{tag}yc", M[jot, j4]); put(f"{tag}yd", M[jot, jsw])
    if "z" in dirs:
        for d in range(-3, 4):
            src = k4 - d; ok = (src >= 0) & (src < 4)
            put(f"{tag}z{d}", np.where(ok, M[k4, np.clip(src, 0, 3)], 0.0))
K4s = K4 / w4[:, None]
for t in ("x", "y", "z"): ops4("a", K4s, t)
put("a0", K4s[i4, i4] + K4s[j4, j4] + K4s[k4, k4])
put("W1", w4[i4] * w4[j4] * w4[k4])
put("G1", Kd4[i4] * w4[j4] * w4[k4] + w4[i4] * Kd4[j4] * w4[k4] + w4[i4] * w4[j4] * Kd4[k4])
put("m1", f4[i4] * f4[j4] * f4[k4])
put("z0", (k4 == 0) * 1.0); put("z3", (k4 == 3) * 1.0)
put("x0", (i4 == 0) * 1.0); put("x3", (i4 == 3) * 1.0)
put("y0", (j4 == 0) * 1.0); put("y3", (j4 == 3) * 1.0)
cor = lambda a: (a == 0) | (a == 3)
cmask = (cor(i4) & cor(j4) & cor(k4)) * 1.0
R2 = np.zeros((4, 4)); R2[0] = J2[:, 0]; R2[3] = J2[:, 1]
P2 = np.zeros((4, 4)); P2[:, 0] = J2[:, 0]; P2[:, 3] = J2[:, 1]
K2s = K2 / w2[:, None]
B2 = np.zeros((4, 4)); B2[np.ix_([0, 3], [0, 3])] = K2s
for t in ("x", "y", "z"):
    ops4("r", R2, t); ops4("p", P2, t); ops4("b", B2, t)
w2e = np.array([w2[0], 0, 0, w2[1]]); Kd2e = np.array([Kd2[0], 0, 0, Kd2[1]])
put("W2", w2e[i4] * w2e[j4] * w2e[k4])
put("G2", Kd2e[i4] * w2e[j4] * w2e[k4] + w2e[i4] * Kd2e[j4] * w2e[k4] + w2e[i4] * w2e[j4] * Kd2e[k4])
put("off2", 1.0 - cmask)
KJ = K8s @ J1
KJx = K8 @ J1
for d in range(-7, 8):
    for hh in range(2):
        src = kz - d; ok = (src >= 0) & (src < 8) & (src % 2 == hh)
        put(f"qz{hh}_{d}", np.where(ok, KJ[kz, np.clip(src // 2, 0, 3)], 0.0))
for b in range(4): put(f"qy{b}", KJ[sub, b] * ones)
for j0 in (0, 7):
    for hh in range(2): put(f"fy{j0}_{hh}", KJ[j0, 2 * jp + (hh ^ jp)] * ones)
for i0 in (0, 7):
    for j0 in (0, 7):
        a0, b0 = (0 if i0 == 0 else 3), (0 if j0 == 0 else 3)
        for hh in range(2):
            b_ = 2 * jp + (hh ^ jp)
            put(f"fc{i0}{j0}_{hh}", (KJ[i0, i4] * (b_ == b0) + KJ[j0, b_] * (i4 == a0)) * ones)
        put(f"fo{i0}{j0}", ((i4 == a0) & (jp == b0 // 2)) * ones)
for q in range(2): put(f"hot{q}", (lane // 8 == sub + 8 * q) * 1.0)
NZ_ = lambda n: np.any(T[n] != 0)
THETA, DELTA = 1.65, 1.35
S_ = THETA / DELTA; rho0 = 1 / S_; rho1 = 1 / (2 * S_ - rho0)
ALPHA = rho1 * rho0; BETA = 2 * rho1 / DELTA

NAMES = [n for n in T if np.any(T[n])]
INDEX = {n: k for k, n in enumerate(NAMES)}
TABLE = np.stack([T[n] for n in NAMES])
K8 = [[float(np.float32(x)) for x in r] for r in K8]
w8 = [float(np.float32(x)) for x in w8]


def live(name):
    return name in INDEX


def lr(v, s):
    return pltpu.roll(v, s % 128, 1)


def sr(v, s):
    return pltpu.roll(v, s % 8, 0)


def halves():
    s = lax.broadcasted_iota(jnp.int32, (8, 128), 0)
    l = lax.broadcasted_iota(jnp.int32, (8, 128), 1)
    return s % 2 == 1, l % 2 == 1

def zops(C, tag, v, skip0=False):
    out = None
    for d in range(-3, 4):
        if (d == 0 and skip0) or not live(f"{tag}z{d}"): continue
        t = C(f"{tag}z{d}") * (lr(v, 2 * d) if d else v)
        out = t if out is None else out + t
    return out

def xops(C, tag, v, skip0=False):
    out = None
    for d in range(4):
        if (d == 0 and skip0) or not live(f"{tag}x{d}"): continue
        t = C(f"{tag}x{d}") * (sr(v, 2 * d) if d else v)
        out = t if out is None else out + t
    return out

def yops(C, tag, v, skip0=False):
    jp1, h1 = halves()
    sw = jnp.where(jp1, sr(v, 1), sr(v, -1)) if live(f"{tag}yb") or live(f"{tag}yd") else None
    def pair(a, b):
        t = None
        if live(a): t = C(a) * v
        if live(b): t = C(b) * sw if t is None else t + C(b) * sw
        return t
    other = pair(f"{tag}yc", f"{tag}yd")
    out = None if other is None else jnp.where(h1, lr(other, 1), lr(other, -1))
    if skip0:
        if live(f"{tag}yb"): out = out + C(f"{tag}yb") * sw
        return out
    same = pair(f"{tag}ya", f"{tag}yb")
    return same if out is None else (out if same is None else out + same)

def a1(C, v, kap, sig):
    k = C("a0") * v + xops(C, "a", v, True) + yops(C, "a", v, True) + zops(C, "a", v, True)
    return C("W1") * (kap * k + sig * v)

def a2(C, v, kap, sig):
    k = xops(C, "b", v) + yops(C, "b", v) + zops(C, "b", v)
    return C("W2") * (kap * k + sig * v)

def restrict2(C, v): return zops(C, "r", yops(C, "r", xops(C, "r", v)))
def prolong2(C, v): return xops(C, "p", yops(C, "p", zops(C, "p", v)))
def sz1(C, v): return v + C("z0") * lr(v, 2) + C("z3") * lr(v, -2)
def xfrom_l(C, v): return C("x0") * sr(v, 2)
def xfrom_r(C, v): return C("x3") * sr(v, -2)
def yfrom_l(C, v): return C("y0") * sr(v, -1)
def yfrom_r(C, v): return C("y3") * sr(v, 1)

def a_fine(C, v, kap, sig, sides):
    kap_y, kap_x, sig_x = sides
    out, to_x, to_y = [], [], []
    for i in range(8):
        t = C("cyz0") * v[i]
        for d in range(1, 8): t = t + C(f"cy{d}") * sr(v[i], d)
        for d in range(-7, 8):
            if d: t = t + C(f"cz{d}") * lr(v[i], d)
        x = K8[i][0] * v[0]
        for a in range(1, 8): x = x + K8[i][a] * v[a]
        o = C("wyz") * (kap * (x + w8[i] * t) + sig * (w8[i] * v[i]))
        out.append(o)
        if i in (0, 7):
            s = i // 7
            to_x.append(o + C("wyz") * (kap_y * x))
            to_y.append(o + C("wyz") * (w8[i] * (kap_x[s] * t + sig_x[s] * v[i])))
    return out, to_x, to_y

def sz8(C, v): return v + C("mz0") * lr(v, 1) + C("mz7") * lr(v, -1)


def scope(name):
    return contextlib.nullcontext()


MESH = pl.DeviceIdType.MESH
NY = 4
ZR = 32
YR = 4
GX = ZR * YR * 2
R = 6
NC = (2 * R + 1) * NY
OWN = R * NY
PARTNERS = [(dx, dy) for far in range(R, -1, -1) for dy in (2, 1, 3, 0) for dx in ((-far, far) if far else (0,)) if (dx, dy) != (0, 0)]
ROUNDS = 7
TI = 1.0 / THETA
NEAR = 3
EDGE = (-R, R)
EDGE_ROWS = {R: (6, 2), -R: (0, 2)}
U_TILES = NC - 1 - 2 * NY + 2 * NY // 4


def slot(dx, dy):
    return (dx + R) * NY + dy % NY


def kernel(tab_hbm, forc_hbm, kap_hbm, sig_hbm, XS, B, R1, coef_out, rel_out,
           tab, forc, kap_in, sig_in, V, ks_s, KS, FS, SC, FR, RC, ID0, D0, Q,
           us, U, ID1, ID2, C1B, D0B, VA, R1B, D1B, VB, C2B, G0B, QB, VC, X1, TMP, Z,
           ap, AZ, pp, AP,
           in_sem, ks_send, kf_send, kf_recv, ks_recv, c_send, c_recv, f_send, f_recv, u_send, u_recv,
           z_send, z_recv, p_send, p_recv, chain):
    gx = lax.axis_index("gx")
    gy = lax.axis_index("gy")
    core = lax.rem(gx, 2)
    zc = lax.rem(gx // 2, ZR)
    yc = gx // (2 * ZR)

    gxs = {dx: lax.rem(gx + dx + GX, GX) for dx in range(-R, R + 1)}
    gys = [lax.rem(gy + dy, NY) for dy in range(NY)]

    def at(dx, dy):
        return (gxs[dx], gys[dy % NY])

    def zring(k):
        return (yc * (2 * ZR) + 2 * lax.rem(zc + k + ZR, ZR) + core, gy)

    def plane(dy, dc, dx):
        return (lax.rem(yc + dy, YR) * (2 * ZR) + 2 * zc + lax.rem(core + dc, 2), lax.rem(gy + dx, NY))

    def C(name):
        return tab[INDEX[name]]

    loads = [pltpu.make_async_copy(a, b, in_sem.at[k]) for k, (a, b) in enumerate(((kap_hbm, kap_in), (sig_hbm, sig_in), (tab_hbm, tab), (forc_hbm, forc)))]
    for c in loads:
        c.start()
    for cyc in range(2):
        for dx in EDGE:
            for dy in range(NY):
                U[cyc, slot(dx, dy)] = jnp.zeros((8, 128), jnp.float32)
    barrier = pltpu.get_barrier_semaphore()
    greet = [at(dx, dy) for dx, dy in PARTNERS if abs(dx) <= NEAR]
    greet += [zring(-1), zring(1), plane(1, 0, 0), plane(3, 0, 0)]
    for d in greet:
        pl.semaphore_signal(barrier, inc=1, device_id=d, device_id_type=MESH)

    with scope('tab_wait'):
        for c in loads:
            c.wait()
    hot = jnp.concatenate([C("hot0"), C("hot1")], axis=0)
    def lanes(ref):
        return jnp.dot(jnp.broadcast_to(ref[...], (8, 16)), hot, precision=lax.Precision.HIGHEST, preferred_element_type=jnp.float32)
    kap = lanes(kap_in)
    sig = lanes(sig_in)
    ks_s[0:1] = kap[0:1]
    ks_s[1:2] = sig[0:1]
    KS[OWN, 0:1] = kap[0:1]
    KS[OWN, 1:2] = sig[0:1]

    def side_copies(rnd):
        to = [at(-1, 0), at(1, 0), at(0, -1), at(0, 1)]
        return [pltpu.make_async_remote_copy(src_ref=FS.at[rnd, n], dst_ref=FR.at[rnd, n ^ 1], send_sem=f_send, recv_sem=f_recv.at[rnd],
                                             device_id=d, device_id_type=MESH) for n, d in enumerate(to)]

    def corner_copies():
        return [pltpu.make_async_remote_copy(src_ref=SC.at[k], dst_ref=RC.at[3 - k], send_sem=c_send, recv_sem=c_recv,
                                             device_id=at(2 * (k // 2) - 1, 2 * (k % 2) - 1), device_id_type=MESH) for k in range(4)]

    def whole(buf, send, recv):
        return pltpu.make_async_remote_copy(src_ref=buf, dst_ref=buf, send_sem=send, recv_sem=recv, device_id=at(1, 0), device_id_type=MESH)

    def keep(tiles):
        for i in range(8):
            V[8 * i:8 * i + 8] = tiles[i]

    def face_start(rnd, to_x, to_y):
        for s in range(2):
            FS[rnd, s] = to_x[s]
            FS[rnd, 2 + s] = V[pl.ds(7 * s, 8, stride=8)]
            if to_y is not None:
                FS[rnd, 2 + s, 0:1] = to_y[0][7 * s:7 * s + 1]
                FS[rnd, 2 + s, 7:8] = to_y[1][7 * s:7 * s + 1]
        with scope('face_start'):
            for c in side_copies(rnd):
                c.start()

    def face_wait(rnd, corners=False):
        with scope('face_wait'):
            whole(FR.at[rnd], f_send, f_recv.at[rnd]).wait_recv()
            if corners:
                whole(RC, c_send, c_recv).wait_recv()
        V[0:8] = V[0:8] + FR[rnd, 0]
        V[56:64] = V[56:64] + FR[rnd, 1]
        for s in range(2):
            V[pl.ds(7 * s, 8, stride=8)] = V[pl.ds(7 * s, 8, stride=8)] + FR[rnd, 2 + s]
        if corners:
            for k, r in enumerate((0, 7, 56, 63)):
                V[r:r + 1] = V[r:r + 1] + RC[k]
        return [V[8 * i:8 * i + 8] for i in range(8)]

    first_v = [sz8(C, forc[i]) for i in range(8)]
    with scope('barrier'):
        pl.semaphore_wait(barrier, len(greet))

    def ks_copy(dx, dy):
        near = abs(dx) <= 1 and dy != 2
        return pltpu.make_async_remote_copy(src_ref=ks_s, dst_ref=KS.at[slot(-dx, -dy)], send_sem=ks_send if near else kf_send,
                                            recv_sem=ks_recv if near else kf_recv, device_id=at(dx, dy), device_id_type=MESH)
    near = [(dx, dy) for dx, dy in PARTNERS if abs(dx) <= 1 and dy != 2]
    far = [p for p in PARTNERS if p not in near]
    for p in near:
        ks_copy(*p).start()
    keep(first_v)
    for k, r in enumerate((0, 7, 56, 63)):
        SC[k] = V[r:r + 1]
    for c in corner_copies():
        c.start()
    face_start(0, (first_v[0], first_v[7]), None)
    def tell(n, to):
        for d in to:
            pl.semaphore_signal(chain.at[n], inc=1, device_id=d, device_id_type=MESH)

    def told(n, count=2):
        pl.semaphore_wait(chain.at[n], count)

    tell(0, (at(-NEAR, 0), at(NEAR, 0)))
    tell(1, (zring(-1), zring(1)))
    tell(5, (plane(1, 0, 0), plane(3, 0, 0)))

    def landed(buf, count, send, recv):
        return pltpu.make_async_remote_copy(src_ref=buf.at[pl.ds(0, count)], dst_ref=buf.at[pl.ds(0, count)], send_sem=send, recv_sem=recv,
                                            device_id=at(1, 0), device_id_type=MESH)

    with scope('ks_wait'):
        landed(KS, len(near), ks_send, ks_recv).wait_recv()

    def row(dx, dy, which):
        return KS[slot(dx, dy), which:which + 1]
    prof = [[], []]
    for dx in (-1, 0, 1):
        for which in range(2):
            prof[which].append(row(dx, 0, which) + C("jm0") * row(dx, -1, which) + C("jm7") * row(dx, 1, which))
    for i in range(8):
        kk, ss = prof[0][1], prof[1][1]
        if i == 0:
            kk, ss = kk + prof[0][0], ss + prof[1][0]
        if i == 7:
            kk, ss = kk + prof[0][2], ss + prof[1][2]
        ii = min(i, 7 - i)
        ID0[i] = 1.0 / sz8(C, kk * C(f"gk{ii}") + ss * C(f"gw{ii}"))

    b = face_wait(0, True)
    told(0)
    with scope('ks_send'):
        for p in far:
            ks_copy(*p).start()
    told(1)
    tell(2, (zring(-2), zring(2)))
    told(5)
    tell(6, (plane(2, 0, 0),))
    for i in range(8):
        B[i] = b[i]
        R1[i] = b[i]
        XS[i] = jnp.zeros((8, 128), jnp.float32)

    def kap_of(dx, dy):
        return KS[(dx + R) * NY + dy, 0:1]

    def sig_of(dx, dy):
        return KS[(dx + R) * NY + dy, 1:2]

    def assembled(buf, dx):
        base = (dx + R) * NY
        u = [buf[base + dy] + xfrom_l(C, buf[base - NY + dy]) + xfrom_r(C, buf[base + NY + dy]) for dy in range(NY)]
        up = [yfrom_l(C, u[dy]) for dy in range(NY)]
        dn = [yfrom_r(C, u[dy]) for dy in range(NY)]
        return [u[dy] + up[(dy - 1) % NY] + dn[(dy + 1) % NY] for dy in range(NY)]

    def over(radius, body):
        for dx in range(-radius, radius + 1):
            body(dx)

    def coarse_diagonals():
        with scope('kf_wait'):
            landed(KS, len(far), kf_send, kf_recv).wait_recv()
        def g_one(dx):
            for dy in range(NY):
                c = (dx + R) * NY + dy
                VA[c] = sz1(C, kap_of(dx, dy) * C("G1") + sig_of(dx, dy) * C("W1"))
                VB[c] = sz1(C, kap_of(dx, dy) * C("G2") + sig_of(dx, dy) * C("W2"))
        with scope('g_one'):
            over(R, g_one)
        def g_two(dx):
            s1, s2 = assembled(VA, dx), assembled(VB, dx)
            for dy in range(NY):
                c = (dx + R) * NY + dy
                ID1[c] = 1.0 / s1[dy]
                ID2[c] = 1.0 / (s2[dy] + C("off2"))
        with scope('g_two'):
            over(R - 1, g_two)

    sides = (C("jm0") * row(0, -1, 0) + C("jm7") * row(0, 1, 0), (row(-1, 0, 0), row(1, 0, 0)), (row(-1, 0, 1), row(1, 0, 1)))

    c1 = kap * C("wyz")
    rho = sig / kap

    def tiles(ref):
        return [ref[i] for i in range(8)]

    def u_copy(cyc, dx, dy):
        rows = pl.ds(*EDGE_ROWS[dx]) if dx in EDGE_ROWS else slice(None)
        return pltpu.make_async_remote_copy(src_ref=us.at[cyc, rows], dst_ref=U.at[cyc, slot(-dx, -dy), rows], send_sem=u_send, recv_sem=u_recv.at[cyc],
                                            device_id=at(dx, dy), device_id_type=MESH)

    def columns(radius):
        return [(dx, dy, (dx + R) * NY + dy) for dx in range(-radius, radius + 1) for dy in range(NY)]

    def sums(buf, radius, put):
        for dx in range(-radius, radius + 1):
            s = assembled(buf, dx)
            for dy in range(NY):
                put((dx + R) * NY + dy, s[dy])

    def image(op, src, dst, radius):
        for dx, dy, c in columns(radius):
            TMP[c] = op(C, src[c], kap_of(dx, dy), sig_of(dx, dy))
        for dx, dy, c in columns(radius):
            dst[c] = sz1(C, TMP[c])

    def coarse(cyc):
        def put1(c, s):
            C1B[c] = s
            D0B[c] = TI * s * ID1[c]
        def put2(c, s):
            r1 = C1B[c] - s
            R1B[c] = r1
            D1B[c] = ALPHA * D0B[c] + BETA * r1 * ID1[c]
        def put3(c, s):
            C2B[c] = s
            G0B[c] = TI * s * ID2[c]
        def put4(c, s):
            QB[c] = (1.0 + ALPHA) * G0B[c] + BETA * (C2B[c] - s) * ID2[c]
        with scope('first'):
            sums(U.at[cyc], R - 1, put1)
            image(a1, D0B, VA, R - 1)
        with scope('second'):
            sums(VA, R - 2, put2)
            for dx, dy, c in columns(R - 2):
                TMP[c] = C("m1") * R1B[c] - a1(C, D1B[c], kap_of(dx, dy), sig_of(dx, dy))
            for dx, dy, c in columns(R - 2):
                TMP[c] = yops(C, "r", xops(C, "r", TMP[c]))
            for dx, dy, c in columns(R - 2):
                TMP[c] = zops(C, "r", TMP[c])
            for dx, dy, c in columns(R - 2):
                VB[c] = sz1(C, TMP[c])
        with scope('third'):
            sums(VB, R - 3, put3)
            image(a2, G0B, VA, R - 3)
        with scope('fourth'):
            sums(VA, R - 4, put4)
            for dx, dy, c in columns(R - 4):
                TMP[c] = zops(C, "p", QB[c])
            for dx, dy, c in columns(R - 4):
                QB[c] = D1B[c] + xops(C, "p", yops(C, "p", TMP[c]))
            image(a1, QB, VC, R - 4)
        with scope('fifth'):
            def put5(c, s):
                X1[c] = D0B[c] + QB[c] + TI * (R1B[c] - s) * ID1[c]
            sums(VC, R - 5, put5)

    def restrict1(t):
        xs = [sum(float(J1[i, a]) * t[i] for i in range(8)) for a in range(4)]
        for s in range(8):
            V[8 * s:8 * s + 8] = xs[s // 2]
        out = None
        for hh in range(2):
            y = None
            for j in range(8):
                if live(f"ry{j}_{hh}"):
                    p = C(f"ry{j}_{hh}") * V[pl.ds(j, 8, stride=8)]
                    y = p if y is None else y + p
            for h2, d in RZ:
                if h2 == hh:
                    p = C(f"rz{hh}_{d}") * (lr(y, d) if d else y)
                    out = p if out is None else out + p
        return out

    around = [(dx, dy) for dx in (-1, 0, 1) for dy in (-1, 0, 1)]

    def lines():
        for n, (dx, dy) in enumerate(around):
            e = X1[slot(dx, dy)]
            z = [None] * 4
            for d in range(-7, 8):
                r = lr(e, d) if d else e
                for hh in range(2):
                    for q, tag in enumerate(("pz", "qz")):
                        if not live(f"{tag}{hh}_{d}"):
                            continue
                        p = C(f"{tag}{hh}_{d}") * r
                        z[2 * q + hh] = p if z[2 * q + hh] is None else z[2 * q + hh] + p
            for q in range(4):
                Z[n, 8 * q:8 * q + 8] = z[q]

    def line(n, q, a, b):
        return Z[n, pl.ds(16 * q + 8 * ((b % 2) ^ (b // 2)) + 2 * a + b // 2, 8, stride=0)]

    def planes(n, a):
        return sum(C(f"py{b}") * line(n, 0, a, b) for b in range(4))

    def planes_image(n, a, rho_n, ex):
        return sum(C(f"qy{b}") * line(n, 0, a, b) + C(f"py{b}") * line(n, 1, a, b) for b in range(4)) + rho_n * ex

    def correction():
        lines()
        rhos = [row(dx, dy, 1) / row(dx, dy, 0) for dx, dy in around]
        ex = [planes(4, a) for a in range(4)]
        ey = [planes_image(4, a, rho, ex[a]) for a in range(4)]
        e = [sum(float(J1[i, a]) * ex[a] for a in range(4)) for i in range(8)]
        for i in range(8):
            V[8 * i:8 * i + 8] = c1 * (sum(float(KJx[i, a]) * ex[a] for a in range(4)) + w8[i] * sum(float(J1[i, a]) * ey[a] for a in range(4)))
        for n, (dx, dy) in enumerate(around):
            kap_n, rho_n = row(dx, dy, 0), rhos[n]
            i0, j0 = (7 if dx < 0 else 0), (7 if dy < 0 else 0)
            a0, b0 = (3 if dx < 0 else 0), (3 if dy < 0 else 0)
            if dx and dy:
                t = C(f"fc{i0}{j0}_0") * Z[n, 0:8] + C(f"fc{i0}{j0}_1") * Z[n, 8:16]
                t = t + C(f"fo{i0}{j0}") * (Z[n, 16:24] + rho_n * Z[n, 0:8])
                t = t + sr(t, 4)
                t = t + sr(t, 2)
                t = t + sr(t, 1)
                r = 8 * (7 - i0) + 7 - j0
                V[r:r + 1] = V[r:r + 1] + (kap_n * (w8[i0] * C("wyz")[0:1] * (w8[j0] / w8[0]))) * t[0:1]
            elif dx:
                q = [planes(n, a) for a in range(4)]
                t = sum(float(KJx[i0, a]) * q[a] for a in range(4)) + w8[i0] * planes_image(n, a0, rho_n, q[a0])
                r = 8 * (7 - i0)
                V[r:r + 8] = V[r:r + 8] + (kap_n * C("wyz")) * t
            elif dy:
                t = C(f"fy{j0}_0") * Z[n, 0:8] + C(f"fy{j0}_1") * Z[n, 8:16]
                t = t + jnp.where(halves()[0], sr(t, 1), sr(t, -1))
                t = t + Z[n, 16:24] + rho_n * Z[n, 0:8]
                Z[n, 32:40] = t
                f = sum(C(f"py{a}") * Z[n, pl.ds(32 + 2 * a + b0 // 2, 8, stride=0)] + C(f"qy{a}") * line(n, 0, a, b0) for a in range(4))
                V[pl.ds(7 - j0, 8, stride=8)] = V[pl.ds(7 - j0, 8, stride=8)] + (kap_n * C("wyz") * w8[j0]) * f
        return e

    def image_start(rnd, v):
        out, to_x, to_y = a_fine(C, v, kap, sig, sides)
        keep([sz8(C, t) for t in out])
        face_start(rnd, [sz8(C, t) for t in to_x], [sz8(C, t) for t in to_y])
        return out

    def apply(rnd, v):
        image_start(rnd, v)
        return face_wait(rnd)

    def cycle(cyc, carry):
        rnd = 1 + 3 * cyc
        r = tiles(R1)
        d0 = [TI * r[i] * ID0[i] for i in range(8)]
        for i in range(8):
            D0[i] = d0[i]
        s = apply(rnd, d0)
        d1, t = [], []
        for i in range(8):
            r1 = R1[i] - s[i]
            R1[i] = r1
            d1.append(ALPHA * D0[i] + BETA * r1 * ID0[i])
            Q[i] = d1[i]
        w, to_x, to_y = a_fine(C, d1, kap, sig, sides)
        t = [float(f8[i]) * C("m8") * R1[i] - w[i] for i in range(8)]
        u = sz1(C, restrict1(t))
        us[cyc] = u
        U[cyc, OWN] = u
        with scope('u_send'):
            for dx, dy in PARTNERS:
                u_copy(cyc, dx, dy).start()
        keep([sz8(C, p) for p in w])
        face_start(rnd + 1, [sz8(C, p) for p in to_x], [sz8(C, p) for p in to_y])
        @pl.when(cyc == 0)
        def _():
            coarse_diagonals()
            told(2)
            tell(3, (zring(-4), zring(4)))
            told(6, 1)
        s = face_wait(rnd + 1)
        for i in range(8):
            R1[i] = R1[i] - s[i]
        with scope('u_wait'):
            landed(U.at[cyc], U_TILES, u_send, u_recv.at[cyc]).wait_recv()
        coarse(cyc)
        @pl.when(cyc == 0)
        def _():
            told(3)
            tell(4, (zring(-8), zring(8)))
        with scope('corr'):
            e = correction()
        for i in range(8):
            Q[i] = Q[i] + e[i]
        s = [sz8(C, V[8 * i:8 * i + 8]) for i in range(8)]
        dl = []
        for i in range(8):
            r3 = R1[i] - s[i]
            R1[i] = r3
            x = TI * r3 * ID0[i]
            dl.append(x)
            XS[i] = XS[i] + (D0[i] + Q[i] + x)
        s = apply(rnd + 2, dl)
        for i in range(8):
            R1[i] = R1[i] - s[i]
        return carry

    lax.fori_loop(0, 2, cycle, 0)

    def dot(p, q):
        t = sum(float(f8[i]) * C("m8") * p[i] * q[i] for i in range(8))
        return jnp.sum(jnp.sum(t, axis=1, keepdims=True), axis=0, keepdims=True)
    ln = lax.broadcasted_iota(jnp.int32, (1, 128), 1)
    mine = jnp.where(ln == 0, dot(B, B), jnp.where(ln == 1, dot(B, R1), dot(R1, R1)))
    ap[...] = mine
    AZ[zc] = mine
    told(4)
    def z_copy(k):
        return pltpu.make_async_remote_copy(src_ref=ap, dst_ref=AZ.at[zc], send_sem=z_send, recv_sem=z_recv, device_id=zring(k), device_id_type=MESH)
    with scope('z_send'):
        for k in range(1, ZR // 2):
            z_copy(k).start()
            z_copy(-k).start()
        z_copy(ZR // 2).start()
    def most(buf, send, recv):
        return pltpu.make_async_remote_copy(src_ref=buf.at[pl.ds(0, 31)], dst_ref=buf.at[pl.ds(0, 31)], send_sem=send, recv_sem=recv,
                                            device_id=at(1, 0), device_id_type=MESH)
    landed(KS, len(near), ks_send, ks_recv).wait_send()
    landed(KS, len(far), kf_send, kf_recv).wait_send()
    for cyc in range(2):
        landed(U.at[cyc], U_TILES, u_send, u_recv.at[cyc]).wait_send()
    whole(FS, f_send, f_recv.at[0]).wait_send()
    whole(SC, c_send, c_recv).wait_send()
    with scope('z_wait'):
        most(AZ, z_send, z_recv).wait_recv()
    part = AZ[0]
    for k in range(1, ZR):
        part = part + AZ[k]
    pp[...] = part
    pi = yc * 8 + gy * 2 + core
    AP[pi] = part
    others = [(a, c, x) for a in range(YR) for c in range(2) for x in range(NY) if (a, c, x) != (0, 0, 0)]
    def p_copy(o):
        return pltpu.make_async_remote_copy(src_ref=pp, dst_ref=AP.at[pi], send_sem=p_send, recv_sem=p_recv, device_id=plane(*o), device_id_type=MESH)
    for o in others:
        p_copy(o).start()
    with scope('p_wait'):
        most(AP, p_send, p_recv).wait_recv()
    tot = AP[0]
    for k in range(1, 32):
        tot = tot + AP[k]
    bb, br, rr = tot[0:1, 0:1], tot[0:1, 1:2], tot[0:1, 2:3]
    ww = bb - 2.0 * br + rr
    coef = (bb - br) / ww
    size = jnp.sqrt((bb * rr - br * br) / (ww * bb))
    coef_out[...] = jnp.broadcast_to(coef, (1, 128))
    rel_out[...] = jnp.broadcast_to(size, (1, 128))

    with scope('send_waits'):
        most(AP, p_send, p_recv).wait_send()
    most(AZ, z_send, z_recv).wait_send()


def solution(mesh):
    f32 = jnp.float32
    col = pltpu.VMEM((NC, 8, 128), f32)
    fine = pltpu.VMEM((8, 8, 128), f32)
    row = pltpu.VMEM((1, 128), f32)
    scratch = [
        pltpu.VMEM((len(NAMES), 8, 128), f32), fine, pltpu.VMEM((1, 16), f32), pltpu.VMEM((1, 16), f32), pltpu.VMEM((64, 128), f32),
        pltpu.VMEM((2, 128), f32), pltpu.VMEM((NC, 2, 128), f32),
        pltpu.VMEM((ROUNDS, 4, 8, 128), f32), pltpu.VMEM((4, 1, 128), f32),
        pltpu.VMEM((ROUNDS, 4, 8, 128), f32), pltpu.VMEM((4, 1, 128), f32),
        fine, fine, fine,
        pltpu.VMEM((2, 8, 128), f32), pltpu.VMEM((2, NC, 8, 128), f32),
        col, col, col, col, col, col, col, col, col, col, col, col, col, col, pltpu.VMEM((9, 40, 128), f32),
        row, pltpu.VMEM((32, 1, 128), f32), row, pltpu.VMEM((32, 1, 128), f32),
        pltpu.SemaphoreType.DMA((4,)),
        pltpu.SemaphoreType.DMA, pltpu.SemaphoreType.DMA, pltpu.SemaphoreType.DMA, pltpu.SemaphoreType.DMA,
        pltpu.SemaphoreType.DMA, pltpu.SemaphoreType.DMA,
        pltpu.SemaphoreType.DMA, pltpu.SemaphoreType.DMA((ROUNDS,)),
        pltpu.SemaphoreType.DMA, pltpu.SemaphoreType.DMA((2,)),
        pltpu.SemaphoreType.DMA, pltpu.SemaphoreType.DMA, pltpu.SemaphoreType.DMA, pltpu.SemaphoreType.DMA,
        pltpu.SemaphoreType.REGULAR((7,)),
    ]
    hbm = pl.BlockSpec(memory_space=pl.ANY)
    call = pl.pallas_call(
        kernel,
        out_shape=[pltpu.VMEM((8, 8, 128), f32)] * 3 + [pltpu.VMEM((1, 128), f32), pltpu.VMEM((1, 128), f32)],
        in_specs=[hbm] * 4,
        out_specs=[pl.BlockSpec(memory_space=pltpu.VMEM)] * 5,
        scratch_shapes=scratch,
        compiler_params=pltpu.CompilerParams(collective_id=0, has_side_effects=True),
        name="helmholtz",
    )
    def local(forcing, kappa, sigma):
        z, b, r, coef, rel = call(jnp.asarray(TABLE), forcing, kappa.reshape(1, 16), sigma.reshape(1, 16))
        coef = coef[None]
        return coef * z, b - coef * (b - r), rel[0, 0]

    return jax.shard_map(local, mesh=mesh, in_specs=(P("gx", "gy", None),) * 3,
                         out_specs=(P("gx", "gy", None), P("gx", "gy", None), P()), check_vma=False)
```

```python
import contextlib

import jax
import jax.numpy as jnp
import numpy as np
from jax import lax
from jax.experimental import pallas as pl
from jax.experimental.pallas import tpu as pltpu
from jax.sharding import PartitionSpec as P


def legendre_table(points, order):
    columns = [points * 0.0 + 1.0, points]
    for degree in range(2, order + 1):
        columns.append(((2 * degree - 1) * points * columns[-1] - (degree - 1) * columns[-2]) / degree)
    return np.stack(columns, axis=1)

def lobatto(count):
    order = count - 1
    points = np.cos(np.pi * np.arange(count) / order)
    for sweep in range(60):
        table = legendre_table(points, order)
        points = points - (points * table[:, order] - table[:, order - 1]) / (count * table[:, order])
    table = legendre_table(points, order)
    weights = 2.0 / (order * count * table[:, order] ** 2)
    values = table[:, order]
    points, weights, values = (points[::-1], weights[::-1], values[::-1])
    spread = points[:, None] - points[None, :] + np.eye(count)
    deriv = values[:, None] / values[None, :] / spread * (1.0 - np.eye(count))
    corner = order * (order + 1) / 4.0
    ends = np.array([-corner] + [0.0] * (count - 2) + [corner])
    return (points, weights, deriv + np.eye(count) * ends[None, :])

def lagrange(fine_points, coarse_points):
    columns = []
    for column in range(len(coarse_points)):
        value = fine_points * 0.0 + 1.0
        for other in range(len(coarse_points)):
            if other != column:
                value = value * (fine_points - coarse_points[other]) / (coarse_points[column] - coarse_points[other])
        columns.append(value)
    return np.stack(columns, axis=1)

X8, w8, D8 = lobatto(8); X4, w4, D4 = lobatto(4); X2, w2, D2 = lobatto(2)
J1 = lagrange(X8, X4)
J2 = lagrange(X4, X2)
K8, K4, K2 = (D.T @ (w[:, None] * D) for D, w in ((D8, w8), (D4, w4), (D2, w2)))
Kd8, Kd4, Kd2 = (np.diag(K) for K in (K8, K4, K2))
f8 = np.array([.5] + [1.]*6 + [.5]); f4 = np.array([.5, 1, 1, .5])
lane = np.arange(128)[None, :]; sub = np.arange(8)[:, None]
ones = np.ones((8, 128))
T = {}
def put(name, a): T[name] = np.ascontiguousarray(np.broadcast_to(a, (8, 128)).astype(np.float32))
kz = lane % 8
K8s = K8 / w8[:, None]
for d in range(1, 8):
    put(f"cy{d}", K8s[sub, (sub - d) % 8] * ones)
for d in range(-7, 8):
    if d == 0: continue
    src = kz - d; ok = (src >= 0) & (src < 8)
    put(f"cz{d}", np.where(ok, K8s[kz, np.clip(src, 0, 7)], 0.0))
put("cyz0", K8s[sub, sub] + K8s[kz, kz])
put("wyz", w8[sub] * w8[kz])
put("mz0", (kz == 0) * 1.0); put("mz7", (kz == 7) * 1.0)
put("jm0", (sub == 0) * 1.0); put("jm7", (sub == 7) * 1.0)
for i in range(4):
    put(f"gk{i}", (Kd8[i] * w8[sub] + w8[i] * Kd8[sub]) * w8[kz] + w8[i] * w8[sub] * Kd8[kz])
    put(f"gw{i}", w8[i] * w8[sub] * w8[kz])
put("m8", f8[sub] * f8[kz])
i4 = sub // 2; jp = sub % 2; h = lane % 2; k4 = (lane % 8) // 2; j4 = 2 * jp + (h ^ jp); jsw = 2 * (1 - jp) + (h ^ (1 - jp)); jot = 2 * jp + ((1 - h) ^ jp)
for j in range(8):
    for hh in range(2):
        put(f"ry{j}_{hh}", J1[j, 2 * jp + (hh ^ jp)] * ones)
RZ = []
for hh in range(2):
    for d in range(-7, 8):
        src = (lane % 8) - d; ok = (src >= 0) & (src < 8) & (h == hh)
        c = np.where(ok, J1[np.clip(src, 0, 7), k4], 0.0)
        if np.any(c != 0): put(f"rz{hh}_{d}", c); RZ.append((hh, d))
PZ = {}
for d in range(-7, 8):
    for hh in range(2):
        src = kz - d; ok = (src >= 0) & (src < 8) & (src % 2 == hh)
        c = np.where(ok, J1[kz, np.clip(src // 2, 0, 3)], 0.0)
        if np.any(c != 0): put(f"pz{hh}_{d}", c); PZ.setdefault(d, []).append(hh)
for b in range(4): put(f"py{b}", J1[sub, b] * ones)
def ops4(tag, M, dirs):
    M = np.asarray(M)
    if "x" in dirs:
        for d in range(4): put(f"{tag}x{d}", M[i4, (i4 - d) % 4] * ones)
    if "y" in dirs:
        put(f"{tag}ya", M[j4, j4]); put(f"{tag}yb", M[j4, jsw])
        put(f"{tag}yc", M[jot, j4]); put(f"{tag}yd", M[jot, jsw])
    if "z" in dirs:
        for d in range(-3, 4):
            src = k4 - d; ok = (src >= 0) & (src < 4)
            put(f"{tag}z{d}", np.where(ok, M[k4, np.clip(src, 0, 3)], 0.0))
K4s = K4 / w4[:, None]
for t in ("x", "y", "z"): ops4("a", K4s, t)
put("a0", K4s[i4, i4] + K4s[j4, j4] + K4s[k4, k4])
put("W1", w4[i4] * w4[j4] * w4[k4])
put("G1", Kd4[i4] * w4[j4] * w4[k4] + w4[i4] * Kd4[j4] * w4[k4] + w4[i4] * w4[j4] * Kd4[k4])
put("m1", f4[i4] * f4[j4] * f4[k4])
put("z0", (k4 == 0) * 1.0); put("z3", (k4 == 3) * 1.0)
put("x0", (i4 == 0) * 1.0); put("x3", (i4 == 3) * 1.0)
put("y0", (j4 == 0) * 1.0); put("y3", (j4 == 3) * 1.0)
cor = lambda a: (a == 0) | (a == 3)
cmask = (cor(i4) & cor(j4) & cor(k4)) * 1.0
R2 = np.zeros((4, 4)); R2[0] = J2[:, 0]; R2[3] = J2[:, 1]
P2 = np.zeros((4, 4)); P2[:, 0] = J2[:, 0]; P2[:, 3] = J2[:, 1]
K2s = K2 / w2[:, None]
B2 = np.zeros((4, 4)); B2[np.ix_([0, 3], [0, 3])] = K2s
for t in ("x", "y", "z"):
    ops4("r", R2, t); ops4("p", P2, t); ops4("b", B2, t)
w2e = np.array([w2[0], 0, 0, w2[1]]); Kd2e = np.array([Kd2[0], 0, 0, Kd2[1]])
put("W2", w2e[i4] * w2e[j4] * w2e[k4])
put("G2", Kd2e[i4] * w2e[j4] * w2e[k4] + w2e[i4] * Kd2e[j4] * w2e[k4] + w2e[i4] * w2e[j4] * Kd2e[k4])
put("off2", 1.0 - cmask)
KJ = K8s @ J1
KJx = K8 @ J1
for d in range(-7, 8):
    for hh in range(2):
        src = kz - d; ok = (src >= 0) & (src < 8) & (src % 2 == hh)
        put(f"qz{hh}_{d}", np.where(ok, KJ[kz, np.clip(src // 2, 0, 3)], 0.0))
for b in range(4): put(f"qy{b}", KJ[sub, b] * ones)
for j0 in (0, 7):
    for hh in range(2): put(f"fy{j0}_{hh}", KJ[j0, 2 * jp + (hh ^ jp)] * ones)
for i0 in (0, 7):
    for j0 in (0, 7):
        a0, b0 = (0 if i0 == 0 else 3), (0 if j0 == 0 else 3)
        for hh in range(2):
            b_ = 2 * jp + (hh ^ jp)
            put(f"fc{i0}{j0}_{hh}", (KJ[i0, i4] * (b_ == b0) + KJ[j0, b_] * (i4 == a0)) * ones)
        put(f"fo{i0}{j0}", ((i4 == a0) & (jp == b0 // 2)) * ones)
for q in range(2): put(f"hot{q}", (lane // 8 == sub + 8 * q) * 1.0)
NZ_ = lambda n: np.any(T[n] != 0)
def z_matrix(tag, skip0):
    m = np.zeros((128, 128), np.float32)
    for d in range(-3, 4):
        if d or not skip0:
            for l in range(128): m[(l - 2 * d) % 128, l] += T[f"{tag}z{d}"][0, l]
    return m
ZM = {"a": z_matrix("a", True), "r": z_matrix("r", False), "p": z_matrix("p", False)}
ZM["q"] = ZM["p"] @ ZM["a"]
ZK = list(ZM)
THETA, DELTA = 1.65, 1.35
S_ = THETA / DELTA; rho0 = 1 / S_; rho1 = 1 / (2 * S_ - rho0)
ALPHA = rho1 * rho0; BETA = 2 * rho1 / DELTA

NAMES = [n for n in T if np.any(T[n])]
INDEX = {n: k for k, n in enumerate(NAMES)}
TABLE = np.stack([T[n] for n in NAMES])
_H = [m.astype(jnp.bfloat16) for m in ZM.values()]
_L = [(m - np.asarray(h, np.float32)).astype(jnp.bfloat16) for m, h in zip(ZM.values(), _H)]
ZTABLE = np.stack([np.tile(np.concatenate([h, l], axis=1), (2, 1)) for h, l in zip(_H, _L)])
K8 = [[float(np.float32(x)) for x in r] for r in K8]
w8 = [float(np.float32(x)) for x in w8]


def live(name):
    return name in INDEX


def lr(v, s):
    return pltpu.roll(v, s % 128, 1)


def sr(v, s):
    return pltpu.roll(v, s % 8, 0)


def halves():
    s = lax.broadcasted_iota(jnp.int32, (8, 128), 0)
    l = lax.broadcasted_iota(jnp.int32, (8, 128), 1)
    return s % 2 == 1, l % 2 == 1

def zops(C, tag, v, skip0=False):
    out = None
    for d in range(-3, 4):
        if (d == 0 and skip0) or not live(f"{tag}z{d}"): continue
        t = C(f"{tag}z{d}") * (lr(v, 2 * d) if d else v)
        out = t if out is None else out + t
    return out

def xops(C, tag, v, skip0=False):
    out = None
    for d in range(4):
        if (d == 0 and skip0) or not live(f"{tag}x{d}"): continue
        t = C(f"{tag}x{d}") * (sr(v, 2 * d) if d else v)
        out = t if out is None else out + t
    return out

def yops(C, tag, v, skip0=False):
    jp1, h1 = halves()
    sw = jnp.where(jp1, sr(v, 1), sr(v, -1)) if live(f"{tag}yb") or live(f"{tag}yd") else None
    def pair(a, b):
        t = None
        if live(a): t = C(a) * v
        if live(b): t = C(b) * sw if t is None else t + C(b) * sw
        return t
    other = pair(f"{tag}yc", f"{tag}yd")
    out = None if other is None else jnp.where(h1, lr(other, 1), lr(other, -1))
    if skip0:
        if live(f"{tag}yb"): out = out + C(f"{tag}yb") * sw
        return out
    same = pair(f"{tag}ya", f"{tag}yb")
    return same if out is None else (out if same is None else out + same)

def a1(C, v, kap, sig, z):
    k = C("a0") * v + xops(C, "a", v, True) + yops(C, "a", v, True) + z
    return C("W1") * (kap * k + sig * v)

def a2(C, v, kap, sig, z=None):
    k = xops(C, "b", v) + yops(C, "b", v) + zops(C, "b", v)
    return C("W2") * (kap * k + sig * v)

def sz1(C, v): return v + C("z0") * lr(v, 2) + C("z3") * lr(v, -2)
def xfrom_l(C, v): return C("x0") * sr(v, 2)
def xfrom_r(C, v): return C("x3") * sr(v, -2)
def yfrom_l(C, v): return C("y0") * sr(v, -1)
def yfrom_r(C, v): return C("y3") * sr(v, 1)

def a_fine(C, v, kap, sig, sides):
    kap_y, kap_x, sig_x = sides
    out, to_x, to_y = [], [], []
    for i in range(8):
        t = C("cyz0") * v[i]
        for d in range(1, 8): t = t + C(f"cy{d}") * sr(v[i], d)
        for d in range(-7, 8):
            if d: t = t + C(f"cz{d}") * lr(v[i], d)
        x = K8[i][0] * v[0]
        for a in range(1, 8): x = x + K8[i][a] * v[a]
        o = C("wyz") * (kap * (x + w8[i] * t) + sig * (w8[i] * v[i]))
        out.append(o)
        if i in (0, 7):
            s = i // 7
            to_x.append(o + C("wyz") * (kap_y * x))
            to_y.append(o + C("wyz") * (w8[i] * (kap_x[s] * t + sig_x[s] * v[i])))
    return out, to_x, to_y

def sz8(C, v): return v + C("mz0") * lr(v, 1) + C("mz7") * lr(v, -1)


def scope(name):
    return contextlib.nullcontext()


MESH = pl.DeviceIdType.MESH
NY = 4
ZR = 32
YR = 4
GX = ZR * YR * 2
R = 6
NC = (2 * R + 1) * NY
OWN = R * NY
PARTNERS = [(dx, dy) for far in range(R, -1, -1) for dy in (2, 1, 3, 0) for dx in ((-far, far) if far else (0,)) if (dx, dy) != (0, 0)]
ROUNDS = 7
TI = 1.0 / THETA
EDGE = (-R, R)
EDGE_ROWS = {R: (6, 2), -R: (0, 2)}
U_TILES = NC - 1 - 2 * NY + 2 * NY // 4


def slot(dx, dy):
    return (dx + R) * NY + dy % NY


def kernel(tab_hbm, zm_hbm, forc_hbm, kap_hbm, sig_hbm, XS, B, R1, coef_out, rel_out,
           tab, zm, forc, kap_in, sig_in, V, ks_s, KS, FS, SC, FR, RC, ID0, D0, Q,
           us, U, ID1, ID2, C1B, D0B, VA, R1B, D1B, VB, C2B, G0B, QB, VC, X1, TMP, ZD, Z,
           ap, AZ, pp, AP,
           in_sem, ks_send, kf_send, kf_recv, ks_recv, c_send, c_recv, f_send, f_recv, u_send, u_recv,
           z_send, z_recv, p_send, p_recv, chain):
    gx = lax.axis_index("gx")
    gy = lax.axis_index("gy")
    core = lax.rem(gx, 2)
    zc = lax.rem(gx // 2, ZR)
    yc = gx // (2 * ZR)

    gxs = {dx: lax.rem(gx + dx + GX, GX) for dx in range(-R, R + 1)}
    gys = [lax.rem(gy + dy, NY) for dy in range(NY)]

    def at(dx, dy):
        return (gxs[dx], gys[dy % NY])

    def zring(k):
        return (yc * (2 * ZR) + 2 * lax.rem(zc + k + ZR, ZR) + core, gy)

    def plane(dy, dc, dx):
        return (lax.rem(yc + dy, YR) * (2 * ZR) + 2 * zc + lax.rem(core + dc, 2), lax.rem(gy + dx, NY))

    def C(name):
        return tab[INDEX[name]]

    loads = [pltpu.make_async_copy(a, b, in_sem.at[k]) for k, (a, b) in enumerate(((kap_hbm, kap_in), (sig_hbm, sig_in), (tab_hbm, tab), (forc_hbm, forc), (zm_hbm, zm)))]
    for c in loads:
        c.start()
    for cyc in range(2):
        for dx in EDGE:
            for dy in range(NY):
                U[cyc, slot(dx, dy)] = jnp.zeros((8, 128), jnp.float32)
    barrier = pltpu.get_barrier_semaphore()
    greet = [at(-3, 0), at(3, 0), at(-2, 0), at(2, 0)] + [at(dx, dy) for dx, dy in PARTNERS if abs(dx) <= 1 and dy != 2]
    greet += [zring(-1), zring(1), plane(1, 0, 0), plane(3, 0, 0)]
    for d in greet:
        pl.semaphore_signal(barrier, inc=1, device_id=d, device_id_type=MESH)

    with scope('tab_wait'):
        for c in loads:
            c.wait()
    hot = jnp.concatenate([C("hot0"), C("hot1")], axis=0)
    def lanes(ref):
        return jnp.dot(jnp.broadcast_to(ref[...], (8, 16)), hot, precision=lax.Precision.HIGHEST, preferred_element_type=jnp.float32)
    kap = lanes(kap_in)
    sig = lanes(sig_in)
    ks_s[0:1] = kap[0:1]
    ks_s[1:2] = sig[0:1]
    KS[OWN, 0:1] = kap[0:1]
    KS[OWN, 1:2] = sig[0:1]

    def side_copies(rnd):
        to = [at(-1, 0), at(1, 0), at(0, -1), at(0, 1)]
        return [pltpu.make_async_remote_copy(src_ref=FS.at[rnd, n], dst_ref=FR.at[rnd, n ^ 1], send_sem=f_send, recv_sem=f_recv.at[rnd],
                                             device_id=d, device_id_type=MESH) for n, d in enumerate(to)]

    def corner_copies():
        return [pltpu.make_async_remote_copy(src_ref=SC.at[k], dst_ref=RC.at[3 - k], send_sem=c_send, recv_sem=c_recv,
                                             device_id=at(2 * (k // 2) - 1, 2 * (k % 2) - 1), device_id_type=MESH) for k in range(4)]

    def whole(buf, send, recv):
        return pltpu.make_async_remote_copy(src_ref=buf, dst_ref=buf, send_sem=send, recv_sem=recv, device_id=at(1, 0), device_id_type=MESH)

    def keep(tiles):
        for i in range(8):
            V[8 * i:8 * i + 8] = tiles[i]

    sublane = lax.broadcasted_iota(jnp.int32, (8, 128), 0)

    def face_start(rnd, tiles, to_x, to_y):
        keep(tiles)
        for s in range(2):
            FS[rnd, s] = sz8(C, to_x[s])
            rows = V[pl.ds(7 * s, 8, stride=8)]
            if to_y is not None:
                a, b = (to_y[0], sr(to_y[1], 7)) if s == 0 else (sr(to_y[0], 1), to_y[1])
                rows = jnp.where(sublane == 0, a, jnp.where(sublane == 7, b, rows))
            FS[rnd, 2 + s] = sz8(C, rows)
        with scope('face_start'):
            for c in side_copies(rnd):
                c.start()
        keep([sz8(C, t) for t in tiles])

    def face_wait(rnd, corners=False):
        with scope('face_wait'):
            whole(FR.at[rnd], f_send, f_recv.at[rnd]).wait_recv()
            if corners:
                whole(RC, c_send, c_recv).wait_recv()
        out = []
        for i in range(8):
            t = V[8 * i:8 * i + 8] + C("jm0") * FR[rnd, 2, i:i + 1] + C("jm7") * FR[rnd, 3, i:i + 1]
            if i in (0, 7):
                t = t + FR[rnd, i // 7]
                if corners:
                    t = t + C("jm0") * RC[2 * (i // 7)] + C("jm7") * RC[2 * (i // 7) + 1]
            out.append(t)
        return out

    first_v = [forc[i] for i in range(8)]
    with scope('barrier'):
        pl.semaphore_wait(barrier, len(greet))

    def ks_copy(dx, dy):
        near = abs(dx) <= 1 and dy != 2
        return pltpu.make_async_remote_copy(src_ref=ks_s, dst_ref=KS.at[slot(-dx, -dy)], send_sem=ks_send if near else kf_send,
                                            recv_sem=ks_recv if near else kf_recv, device_id=at(dx, dy), device_id_type=MESH)
    near = [(dx, dy) for dx, dy in PARTNERS if abs(dx) <= 1 and dy != 2]
    far = [p for p in PARTNERS if p not in near]
    far1 = [p for p in far if abs(p[0]) <= (2 if p[1] == 2 else 4) or p[1] == 0]
    far2 = [p for p in far if p not in far1]

    def ks_to(group):
        with scope('ks_send'):
            for p in group:
                ks_copy(*p).start()

    ks_to(near)
    for k, (i, r) in enumerate(((0, 0), (0, 7), (7, 0), (7, 7))):
        SC[k] = sz8(C, first_v[i])[r:r + 1]
    for c in corner_copies():
        c.start()
    face_start(0, first_v, (first_v[0], first_v[7]), None)
    def tell(n, to):
        for d in to:
            pl.semaphore_signal(chain.at[n], inc=1, device_id=d, device_id_type=MESH)

    def told(n, count=2):
        pl.semaphore_wait(chain.at[n], count)

    tell(0, (at(-3, 0), at(3, 0)))
    tell(1, (zring(-1), zring(1)))
    tell(5, (plane(1, 0, 0), plane(3, 0, 0)))

    def landed(buf, count, send, recv):
        return pltpu.make_async_remote_copy(src_ref=buf.at[pl.ds(0, count)], dst_ref=buf.at[pl.ds(0, count)], send_sem=send, recv_sem=recv,
                                            device_id=at(1, 0), device_id_type=MESH)

    with scope('ks_wait'):
        landed(KS, len(near), ks_send, ks_recv).wait_recv()

    def row(dx, dy, which):
        return KS[slot(dx, dy), which:which + 1]
    prof = [[], []]
    for dx in (-1, 0, 1):
        for which in range(2):
            prof[which].append(row(dx, 0, which) + C("jm0") * row(dx, -1, which) + C("jm7") * row(dx, 1, which))
    for i in range(8):
        kk, ss = prof[0][1], prof[1][1]
        if i == 0:
            kk, ss = kk + prof[0][0], ss + prof[1][0]
        if i == 7:
            kk, ss = kk + prof[0][2], ss + prof[1][2]
        ii = min(i, 7 - i)
        ID0[i] = 1.0 / sz8(C, kk * C(f"gk{ii}") + ss * C(f"gw{ii}"))

    b = face_wait(0, True)
    told(0)
    tell(7, (at(-5, 0), at(5, 0)))
    ks_to(far1)
    for i in range(8):
        B[i] = b[i]
        R1[i] = b[i]
        XS[i] = jnp.zeros((8, 128), jnp.float32)

    def kap_of(dx, dy):
        return KS[(dx + R) * NY + dy, 0:1]

    def sig_of(dx, dy):
        return KS[(dx + R) * NY + dy, 1:2]

    def assembled(buf, dx):
        base = (dx + R) * NY
        u = [buf[base + dy] + xfrom_l(C, buf[base - NY + dy]) + xfrom_r(C, buf[base + NY + dy]) for dy in range(NY)]
        up = [yfrom_l(C, u[dy]) for dy in range(NY)]
        dn = [yfrom_r(C, u[dy]) for dy in range(NY)]
        return [u[dy] + up[(dy - 1) % NY] + dn[(dy + 1) % NY] for dy in range(NY)]

    def over(radius, body):
        for dx in range(-radius, radius + 1):
            body(dx)

    def coarse_diagonals():
        with scope('kf_wait'):
            landed(KS, len(far), kf_send, kf_recv).wait_recv()
        def g_one(dx):
            for dy in range(NY):
                c = (dx + R) * NY + dy
                VA[c] = sz1(C, kap_of(dx, dy) * C("G1") + sig_of(dx, dy) * C("W1"))
                VB[c] = sz1(C, kap_of(dx, dy) * C("G2") + sig_of(dx, dy) * C("W2"))
        with scope('g_one'):
            over(R, g_one)
        def g_two(dx):
            s1, s2 = assembled(VA, dx), assembled(VB, dx)
            for dy in range(NY):
                c = (dx + R) * NY + dy
                ID1[c] = 1.0 / s1[dy]
                ID2[c] = 1.0 / (s2[dy] + C("off2"))
        with scope('g_two'):
            over(R - 1, g_two)

    sides = (C("jm0") * row(0, -1, 0) + C("jm7") * row(0, 1, 0), (row(-1, 0, 0), row(1, 0, 0)), (row(-1, 0, 1), row(1, 0, 1)))

    c1 = kap * C("wyz")
    rho = sig / kap

    def tiles(ref):
        return [ref[i] for i in range(8)]

    def u_copy(cyc, dx, dy):
        rows = pl.ds(*EDGE_ROWS[dx]) if dx in EDGE_ROWS else slice(None)
        return pltpu.make_async_remote_copy(src_ref=us.at[cyc, rows], dst_ref=U.at[cyc, slot(-dx, -dy), rows], send_sem=u_send, recv_sem=u_recv.at[cyc],
                                            device_id=at(dx, dy), device_id_type=MESH)

    def columns(radius):
        return [(dx, dy, (dx + R) * NY + dy) for dx in range(-radius, radius + 1) for dy in range(NY)]

    def sums(buf, radius, put):
        for dx in range(-radius, radius + 1):
            s = assembled(buf, dx)
            for dy in range(NY):
                put((dx + R) * NY + dy, s[dy])

    def along_z(src, radius, *tags):
        lo, n = (R - radius) * NY, (2 * radius + 1) * NY
        v = src[lo:lo + n].reshape(n * 8, 128)
        high = v.astype(jnp.bfloat16)
        low = (v - high.astype(jnp.float32)).astype(jnp.bfloat16)
        both = jnp.concatenate([high, low], axis=1)
        out = []
        for tag in tags:
            p = jnp.dot(both, zm[ZK.index(tag)], preferred_element_type=jnp.float32)
            out.append((p[:, 0:128] + p[:, 128:256]).reshape(n, 8, 128))
        return out

    def image(op, src, dst, radius, tag=None):
        z = along_z(src, radius, tag)[0] if tag else None
        for n, (dx, dy, c) in enumerate(columns(radius)):
            TMP[c] = op(C, src[c], kap_of(dx, dy), sig_of(dx, dy), z[n] if tag else None)
        for dx, dy, c in columns(radius):
            dst[c] = sz1(C, TMP[c])

    def coarse(cyc):
        def put1(c, s):
            C1B[c] = s
            D0B[c] = TI * s * ID1[c]
        def put2(c, s):
            r1 = C1B[c] - s
            R1B[c] = r1
            D1B[c] = ALPHA * D0B[c] + BETA * r1 * ID1[c]
        def put3(c, s):
            C2B[c] = s
            G0B[c] = TI * s * ID2[c]
        def put4(c, s):
            QB[c] = (1.0 + ALPHA) * G0B[c] + BETA * (C2B[c] - s) * ID2[c]
        with scope('first'):
            sums(U.at[cyc], R - 1, put1)
            image(a1, D0B, VA, R - 1, 'a')
        with scope('second'):
            sums(VA, R - 2, put2)
            z, = along_z(D1B, R - 2, "a")
            for n, (dx, dy, c) in enumerate(columns(R - 2)):
                TMP[c] = C("m1") * R1B[c] - a1(C, D1B[c], kap_of(dx, dy), sig_of(dx, dy), z[n])
                if abs(dx) <= R - 4:
                    ZD[c] = z[n]
            for dx, dy, c in columns(R - 2):
                TMP[c] = yops(C, "r", xops(C, "r", TMP[c]))
            z, = along_z(TMP, R - 2, "r")
            for n, (dx, dy, c) in enumerate(columns(R - 2)):
                VB[c] = sz1(C, z[n])
        with scope('third'):
            sums(VB, R - 3, put3)
            image(a2, G0B, VA, R - 3)
        with scope('fourth'):
            sums(VA, R - 4, put4)
            zp, zq = along_z(QB, R - 4, "p", "q")
            for n, (dx, dy, c) in enumerate(columns(R - 4)):
                q = D1B[c] + xops(C, "p", yops(C, "p", zp[n]))
                z = ZD[c] + xops(C, "p", yops(C, "p", zq[n]))
                QB[c] = q
                TMP[c] = a1(C, q, kap_of(dx, dy), sig_of(dx, dy), z)
            for dx, dy, c in columns(R - 4):
                VC[c] = sz1(C, TMP[c])
        with scope('fifth'):
            def put5(c, s):
                X1[c] = D0B[c] + QB[c] + TI * (R1B[c] - s) * ID1[c]
            sums(VC, R - 5, put5)

    def restrict1(t):
        xs = [sum(float(J1[i, a]) * t[i] for i in range(8)) for a in range(4)]
        for s in range(8):
            V[8 * s:8 * s + 8] = xs[s // 2]
        out = None
        for hh in range(2):
            y = None
            for j in range(8):
                if live(f"ry{j}_{hh}"):
                    p = C(f"ry{j}_{hh}") * V[pl.ds(j, 8, stride=8)]
                    y = p if y is None else y + p
            for h2, d in RZ:
                if h2 == hh:
                    p = C(f"rz{hh}_{d}") * (lr(y, d) if d else y)
                    out = p if out is None else out + p
        return out

    around = [(dx, dy) for dx in (-1, 0, 1) for dy in (-1, 0, 1)]

    def lines():
        for n, (dx, dy) in enumerate(around):
            e = X1[slot(dx, dy)]
            z = [None] * 4
            for d in range(-7, 8):
                r = lr(e, d) if d else e
                for hh in range(2):
                    for q, tag in enumerate(("pz", "qz")):
                        if not live(f"{tag}{hh}_{d}"):
                            continue
                        p = C(f"{tag}{hh}_{d}") * r
                        z[2 * q + hh] = p if z[2 * q + hh] is None else z[2 * q + hh] + p
            for q in range(4):
                Z[n, 8 * q:8 * q + 8] = z[q]

    def line(n, q, a, b):
        return Z[n, pl.ds(16 * q + 8 * ((b % 2) ^ (b // 2)) + 2 * a + b // 2, 8, stride=0)]

    def planes(n, a):
        return sum(C(f"py{b}") * line(n, 0, a, b) for b in range(4))

    def planes_image(n, a, rho_n, ex):
        return sum(C(f"qy{b}") * line(n, 0, a, b) + C(f"py{b}") * line(n, 1, a, b) for b in range(4)) + rho_n * ex

    def correction():
        lines()
        rhos = [row(dx, dy, 1) / row(dx, dy, 0) for dx, dy in around]
        ex = [planes(4, a) for a in range(4)]
        ey = [planes_image(4, a, rho, ex[a]) for a in range(4)]
        e = [sum(float(J1[i, a]) * ex[a] for a in range(4)) for i in range(8)]
        for i in range(8):
            V[8 * i:8 * i + 8] = c1 * (sum(float(KJx[i, a]) * ex[a] for a in range(4)) + w8[i] * sum(float(J1[i, a]) * ey[a] for a in range(4)))
        for n, (dx, dy) in enumerate(around):
            kap_n, rho_n = row(dx, dy, 0), rhos[n]
            i0, j0 = (7 if dx < 0 else 0), (7 if dy < 0 else 0)
            a0, b0 = (3 if dx < 0 else 0), (3 if dy < 0 else 0)
            if dx and dy:
                t = C(f"fc{i0}{j0}_0") * Z[n, 0:8] + C(f"fc{i0}{j0}_1") * Z[n, 8:16]
                t = t + C(f"fo{i0}{j0}") * (Z[n, 16:24] + rho_n * Z[n, 0:8])
                t = t + sr(t, 4)
                t = t + sr(t, 2)
                t = t + sr(t, 1)
                r = 8 * (7 - i0) + 7 - j0
                V[r:r + 1] = V[r:r + 1] + (kap_n * (w8[i0] * C("wyz")[0:1] * (w8[j0] / w8[0]))) * t[0:1]
            elif dx:
                q = [planes(n, a) for a in range(4)]
                t = sum(float(KJx[i0, a]) * q[a] for a in range(4)) + w8[i0] * planes_image(n, a0, rho_n, q[a0])
                r = 8 * (7 - i0)
                V[r:r + 8] = V[r:r + 8] + (kap_n * C("wyz")) * t
            elif dy:
                t = C(f"fy{j0}_0") * Z[n, 0:8] + C(f"fy{j0}_1") * Z[n, 8:16]
                t = t + jnp.where(halves()[0], sr(t, 1), sr(t, -1))
                t = t + Z[n, 16:24] + rho_n * Z[n, 0:8]
                Z[n, 32:40] = t
                f = sum(C(f"py{a}") * Z[n, pl.ds(32 + 2 * a + b0 // 2, 8, stride=0)] + C(f"qy{a}") * line(n, 0, a, b0) for a in range(4))
                V[pl.ds(7 - j0, 8, stride=8)] = V[pl.ds(7 - j0, 8, stride=8)] + (kap_n * C("wyz") * w8[j0]) * f
        return e

    def image_start(rnd, v):
        face_start(rnd, *a_fine(C, v, kap, sig, sides))

    def cycle(cyc, carry):
        rnd = 1 + 3 * cyc
        r = tiles(R1)
        d0 = [TI * r[i] * ID0[i] for i in range(8)]
        for i in range(8):
            D0[i] = d0[i]
        image_start(rnd, d0)
        @pl.when(cyc == 0)
        def _():
            told(1)
            tell(2, (zring(-2), zring(2)))
            told(5)
            tell(6, (plane(2, 0, 0),))
            told(7)
            ks_to(far2)
        s = face_wait(rnd)
        d1, t = [], []
        for i in range(8):
            r1 = R1[i] - s[i]
            R1[i] = r1
            d1.append(ALPHA * D0[i] + BETA * r1 * ID0[i])
            Q[i] = d1[i]
        w, to_x, to_y = a_fine(C, d1, kap, sig, sides)
        t = [float(f8[i]) * C("m8") * R1[i] - w[i] for i in range(8)]
        u = sz1(C, restrict1(t))
        us[cyc] = u
        U[cyc, OWN] = u
        with scope('u_send'):
            for dx, dy in PARTNERS:
                u_copy(cyc, dx, dy).start()
        face_start(rnd + 1, w, to_x, to_y)
        @pl.when(cyc == 0)
        def _():
            told(2)
            tell(3, (zring(-4), zring(4)))
            coarse_diagonals()
            told(6, 1)
        s = face_wait(rnd + 1)
        for i in range(8):
            R1[i] = R1[i] - s[i]
        with scope('u_wait'):
            landed(U.at[cyc], U_TILES, u_send, u_recv.at[cyc]).wait_recv()
        coarse(cyc)
        with scope('corr'):
            e = correction()
        for i in range(8):
            Q[i] = Q[i] + e[i]
        s = [sz8(C, V[8 * i:8 * i + 8]) for i in range(8)]
        dl = []
        for i in range(8):
            r3 = R1[i] - s[i]
            R1[i] = r3
            x = TI * r3 * ID0[i]
            dl.append(x)
            XS[i] = XS[i] + (D0[i] + Q[i] + x)
        image_start(rnd + 2, dl)
        s = face_wait(rnd + 2)
        @pl.when(cyc == 0)
        def _():
            told(3)
            tell(4, (zring(-8), zring(8)))
        for i in range(8):
            R1[i] = R1[i] - s[i]
        return carry

    lax.fori_loop(0, 2, cycle, 0)

    def dot(p, q):
        t = sum(float(f8[i]) * C("m8") * p[i] * q[i] for i in range(8))
        return jnp.sum(jnp.sum(t, axis=1, keepdims=True), axis=0, keepdims=True)
    ln = lax.broadcasted_iota(jnp.int32, (1, 128), 1)
    mine = jnp.where(ln == 0, dot(B, B), jnp.where(ln == 1, dot(B, R1), dot(R1, R1)))
    ap[...] = mine
    AZ[zc] = mine
    told(4)
    def z_copy(k):
        return pltpu.make_async_remote_copy(src_ref=ap, dst_ref=AZ.at[zc], send_sem=z_send, recv_sem=z_recv, device_id=zring(k), device_id_type=MESH)
    with scope('z_send'):
        for k in range(1, ZR // 2):
            z_copy(k).start()
            z_copy(-k).start()
        z_copy(ZR // 2).start()
    def most(buf, send, recv):
        return pltpu.make_async_remote_copy(src_ref=buf.at[pl.ds(0, 31)], dst_ref=buf.at[pl.ds(0, 31)], send_sem=send, recv_sem=recv,
                                            device_id=at(1, 0), device_id_type=MESH)
    landed(KS, len(near), ks_send, ks_recv).wait_send()
    landed(KS, len(far), kf_send, kf_recv).wait_send()
    for cyc in range(2):
        landed(U.at[cyc], U_TILES, u_send, u_recv.at[cyc]).wait_send()
    whole(FS, f_send, f_recv.at[0]).wait_send()
    whole(SC, c_send, c_recv).wait_send()
    with scope('z_wait'):
        most(AZ, z_send, z_recv).wait_recv()
    part = AZ[0]
    for k in range(1, ZR):
        part = part + AZ[k]
    pp[...] = part
    pi = yc * 8 + gy * 2 + core
    AP[pi] = part
    others = [(a, c, x) for a in range(YR) for c in range(2) for x in range(NY) if (a, c, x) != (0, 0, 0)]
    def p_copy(o):
        return pltpu.make_async_remote_copy(src_ref=pp, dst_ref=AP.at[pi], send_sem=p_send, recv_sem=p_recv, device_id=plane(*o), device_id_type=MESH)
    for o in others:
        p_copy(o).start()
    with scope('p_wait'):
        most(AP, p_send, p_recv).wait_recv()
    tot = AP[0]
    for k in range(1, 32):
        tot = tot + AP[k]
    bb, br, rr = tot[0:1, 0:1], tot[0:1, 1:2], tot[0:1, 2:3]
    ww = bb - 2.0 * br + rr
    coef = (bb - br) / ww
    size = jnp.sqrt((bb * rr - br * br) / (ww * bb))
    coef_out[...] = jnp.broadcast_to(coef, (1, 128))
    rel_out[...] = jnp.broadcast_to(size, (1, 128))

    with scope('send_waits'):
        most(AP, p_send, p_recv).wait_send()
    most(AZ, z_send, z_recv).wait_send()


def solution(mesh):
    f32 = jnp.float32
    col = pltpu.VMEM((NC, 8, 128), f32)
    fine = pltpu.VMEM((8, 8, 128), f32)
    row = pltpu.VMEM((1, 128), f32)
    scratch = [
        pltpu.VMEM((len(NAMES), 8, 128), f32), pltpu.VMEM((len(ZK), 256, 256), jnp.bfloat16), fine, pltpu.VMEM((1, 16), f32), pltpu.VMEM((1, 16), f32), pltpu.VMEM((64, 128), f32),
        pltpu.VMEM((2, 128), f32), pltpu.VMEM((NC, 2, 128), f32),
        pltpu.VMEM((ROUNDS, 4, 8, 128), f32), pltpu.VMEM((4, 1, 128), f32),
        pltpu.VMEM((ROUNDS, 4, 8, 128), f32), pltpu.VMEM((4, 1, 128), f32),
        fine, fine, fine,
        pltpu.VMEM((2, 8, 128), f32), pltpu.VMEM((2, NC, 8, 128), f32),
        col, col, col, col, col, col, col, col, col, col, col, col, col, col, col, pltpu.VMEM((9, 40, 128), f32),
        row, pltpu.VMEM((32, 1, 128), f32), row, pltpu.VMEM((32, 1, 128), f32),
        pltpu.SemaphoreType.DMA((5,)),
        pltpu.SemaphoreType.DMA, pltpu.SemaphoreType.DMA, pltpu.SemaphoreType.DMA, pltpu.SemaphoreType.DMA,
        pltpu.SemaphoreType.DMA, pltpu.SemaphoreType.DMA,
        pltpu.SemaphoreType.DMA, pltpu.SemaphoreType.DMA((ROUNDS,)),
        pltpu.SemaphoreType.DMA, pltpu.SemaphoreType.DMA((2,)),
        pltpu.SemaphoreType.DMA, pltpu.SemaphoreType.DMA, pltpu.SemaphoreType.DMA, pltpu.SemaphoreType.DMA,
        pltpu.SemaphoreType.REGULAR((8,)),
    ]
    hbm = pl.BlockSpec(memory_space=pl.ANY)
    call = pl.pallas_call(
        kernel,
        out_shape=[pltpu.VMEM((8, 8, 128), f32)] * 3 + [pltpu.VMEM((1, 128), f32), pltpu.VMEM((1, 128), f32)],
        in_specs=[hbm] * 5,
        out_specs=[pl.BlockSpec(memory_space=pltpu.VMEM)] * 5,
        scratch_shapes=scratch,
        compiler_params=pltpu.CompilerParams(collective_id=0, has_side_effects=True),
        name="helmholtz",
    )
    def local(forcing, kappa, sigma):
        z, b, r, coef, rel = call(jnp.asarray(TABLE), jnp.asarray(ZTABLE), forcing, kappa.reshape(1, 16), sigma.reshape(1, 16))
        coef = coef[None]
        return coef * z, b - coef * (b - r), rel[0, 1]

    return jax.shard_map(local, mesh=mesh, in_specs=(P("gx", "gy", None),) * 3,
                         out_specs=(P("gx", "gy", None), P("gx", "gy", None), P()), check_vma=False)
```
